128 devices in a mesh: stage: 1, model: 16 (over z, y), data: 8 (over x, core).
Axes of the slice: x: 4, y: 4, z: 4, core: 2. Of those that a mesh axis runs over, the one named last changes fastest.
Arguments:
- w_fc1: float32 [16, 1024, 1024], P('stage', 'data', 'model')
- m_fc1: float32 [16, 1024, 1024], P('stage', 'data', 'model')
- g_fc1: bfloat16 [16, 1024, 1024], P('stage', 'data', 'model')
- w_fc2: float32 [16, 1024, 512], P('stage', 'data', 'model')
- m_fc2: float32 [16, 1024, 512], P('stage', 'data', 'model')
- g_fc2: bfloat16 [16, 1024, 512], P('stage', 'data', 'model')
Outputs:
- output 1: float32 [16, 1024, 1024], P('stage', 'data', 'model')
- output 2: float32 [16, 1024, 1024], P('stage', 'data', 'model')
- output 3: float32 [16, 1024, 512], P('stage', 'data', 'model')
- output 4: float32 [16, 1024, 512], P('stage', 'data', 'model')
All inputs are finite; a program needn't handle non-finite values.
Results may differ from the reference program's by a relative error of at most 0.00763347.
Values are sent between devices in bfloat16 or wider.
A program may use at most 1 GiB of HBM per device.

```python
import math
import jax
import jax.numpy as jnp
from jax import lax

HIDDEN = 1024
EXPERT_FFN = 512
EXPERTS = 16
NS_STEPS = 5
LOW_RANK = 4

NS_COEF_A = 3.4445
NS_COEF_B = -4.7750
NS_COEF_C = 2.0315
MOMENTUM = 0.95
LEARN_RATE = 0.04
DECAY = 0.2
NORM_EPS = 1e-7


def draw_state(key, cols):
    key_noise, key_left, key_right, key_scale = jax.random.split(key, 4)
    noise = jax.random.normal(key_noise, (EXPERTS, HIDDEN, cols), jnp.float32)
    left = jax.random.normal(key_left, (EXPERTS, HIDDEN, LOW_RANK), jnp.float32)
    right = jax.random.normal(key_right, (EXPERTS, LOW_RANK, cols), jnp.float32)
    shared = jnp.einsum('emr,ern->emn', left, right) / math.sqrt(LOW_RANK)
    row_scale = jax.random.uniform(key_scale, (EXPERTS, HIDDEN, 1), jnp.float32, 0.5, 1.5)
    return row_scale * (noise + shared) * math.sqrt(0.5)


def setup_inputs(seed: int = 0, part: int = 0) -> dict:
    base = jax.random.fold_in(jax.random.key(seed), part)
    keys = jax.random.split(base, 6)
    fc1_cols = 2 * EXPERT_FFN
    w_scale = HIDDEN ** -0.5
    return {
        'w_fc1': jax.random.normal(keys[0], (EXPERTS, HIDDEN, fc1_cols), jnp.float32) * w_scale,
        'm_fc1': draw_state(keys[1], fc1_cols),
        'g_fc1': draw_state(keys[2], fc1_cols).astype(jnp.bfloat16),
        'w_fc2': jax.random.normal(keys[3], (EXPERTS, HIDDEN, EXPERT_FFN), jnp.float32) * w_scale,
        'm_fc2': draw_state(keys[4], EXPERT_FFN),
        'g_fc2': draw_state(keys[5], EXPERT_FFN).astype(jnp.bfloat16),
    }


def orthogonalize(momentum):
    row_count, col_count = momentum.shape
    norm_val = jnp.sqrt(jnp.sum(momentum * momentum))
    x_mat = (momentum.astype(jnp.bfloat16).astype(jnp.float32) / (norm_val + NORM_EPS)).astype(jnp.bfloat16)
    if row_count > col_count:
        x_mat = x_mat.T
    for ns_step in range(NS_STEPS):
        gram_mat = jnp.dot(x_mat, x_mat.T, preferred_element_type=jnp.float32).astype(jnp.bfloat16)
        gram_sq = jnp.dot(gram_mat, gram_mat, preferred_element_type=jnp.float32)
        poly_mat = (NS_COEF_B * gram_mat.astype(jnp.float32) + NS_COEF_C * gram_sq).astype(jnp.bfloat16)
        update_term = jnp.dot(poly_mat, x_mat, preferred_element_type=jnp.float32)
        x_mat = (NS_COEF_A * x_mat.astype(jnp.float32) + update_term).astype(jnp.bfloat16)
    if row_count > col_count:
        x_mat = x_mat.T
    return x_mat.astype(jnp.float32) * (0.2 * math.sqrt(max(row_count, col_count)))


def update_stack(weights, momentum, gradient):
    new_mom = MOMENTUM * momentum + gradient.astype(jnp.float32)
    ortho = lax.map(orthogonalize, new_mom)
    new_w = weights - LEARN_RATE * (ortho + DECAY * weights)
    return new_w, new_mom


def reference(w_fc1, m_fc1, g_fc1, w_fc2, m_fc2, g_fc2):
    new_w1, new_m1 = update_stack(w_fc1, m_fc1, g_fc1)
    new_w2, new_m2 = update_stack(w_fc2, m_fc2, g_fc2)
    return (new_w1, new_m1, new_w2, new_m2)
```

```python
import functools
import math
import jax
import jax.numpy as jnp
from jax import lax
from jax.experimental import pallas as pl
from jax.experimental.pallas import tpu as pltpu
from jax.sharding import PartitionSpec as P

NS_STEPS = 5
NS_COEF_A = 3.4445
NS_COEF_B = -4.7750
NS_COEF_C = 2.0315
MOMENTUM = 0.95
LEARN_RATE = 0.04
DECAY = 0.2
NORM_EPS = 1e-7

BF16 = jnp.bfloat16
F32 = jnp.float32
NN = ((1,), (0,))
TN = ((0,), (0,))
NT = ((1,), (1,))
MESH = pl.DeviceIdType.MESH


def dot(lhs, rhs, dims):
    return lax.dot_general(lhs, rhs, (dims, ((), ())), preferred_element_type=F32)


def muon_kernel(m1_hbm, g1_hbm, m2_hbm, g2_hbm, res1, res2,
                m1, g1, m2, g2, send1, send2, part1, part2,
                raw1, raw2, norms, y_own, y_oth, a_own, a_cross, a_oth, b_own, b_cross, y2, a2, b2,
                in_sem, send_sem, gather_sem, norm_sem, result_sem, y_send, y_recv, a_send, a_recv, out_send):
    midx = lax.axis_index('model')
    didx = lax.axis_index('data')
    core = didx % 2
    xpos = didx // 2
    diag = midx // 4 + midx % 4
    flat = midx * 8 + didx
    is_own1 = (8 - diag) % 4 == xpos
    is_own2 = jnp.logical_and((10 - diag) % 4 == xpos, core == 1)

    def to(model, data):
        return {'model': model, 'data': data}

    loads = [pltpu.make_async_copy(src, dst, in_sem.at[i])
             for i, (src, dst) in enumerate(((m1_hbm, m1), (g1_hbm, g1), (m2_hbm, m2), (g2_hbm, g2)))]
    for load in loads:
        load.start()

    barrier = pltpu.get_barrier_semaphore()

    def greet(i, carry):
        other = (flat + i) % 128
        pl.semaphore_signal(barrier, inc=1, device_id=to(other // 8, other % 8), device_id_type=MESH)
        return carry

    lax.fori_loop(1, 128, greet, 0)

    def momentum(e, carry, m_ref, g_ref, send, part):
        value = MOMENTUM * m_ref[e] + g_ref[e].astype(F32)
        send[e] = value.astype(BF16)
        part[e] = jnp.sum(value * value, axis=0, keepdims=True)
        return carry

    loads[0].wait()
    loads[1].wait()
    lax.fori_loop(0, 16, functools.partial(momentum, m_ref=m1, g_ref=g1, send=send1, part=part1), 0)
    loads[2].wait()
    loads[3].wait()
    lax.fori_loop(0, 16, functools.partial(momentum, m_ref=m2, g_ref=g2, send=send2, part=part2), 0)
    pl.semaphore_wait(barrier, 127)

    def send_fc1(i, carry):
        e = (midx + 2 * didx + i) % 16
        ox = (8 - e // 4 - e % 4) % 4
        mine = jnp.logical_and(e == midx, is_own1)
        for side in range(2):
            @pl.when(jnp.logical_not(jnp.logical_and(mine, core == side)))
            def _():
                pltpu.make_async_remote_copy(
                    part1.at[e], norms.at[flat], send_sem.at[1], norm_sem,
                    device_id=to(e, 2 * ox + side), device_id_type=MESH).start()

        @pl.when(jnp.logical_not(mine))
        def _():
            pltpu.make_async_remote_copy(
                send1.at[e], raw1.at[xpos * 16 + midx], send_sem.at[0], gather_sem.at[xpos // 2],
                device_id=to(e, 2 * ox + core), device_id_type=MESH).start()
        return carry

    lax.fori_loop(0, 16, send_fc1, 0)

    def send_fc2(i, carry):
        e = (midx + 2 * didx + i) % 16
        ox = (10 - e // 4 - e % 4) % 4

        @pl.when(jnp.logical_not(jnp.logical_and(e == midx, is_own2)))
        def _():
            pltpu.make_async_remote_copy(
                part2.at[e], norms.at[flat], send_sem.at[3], norm_sem,
                device_id=to(e, 2 * ox + 1), device_id_type=MESH).start()
            pltpu.make_async_remote_copy(
                send2.at[e], raw2.at[flat], send_sem.at[2], gather_sem.at[0],
                device_id=to(e, 2 * ox + 1), device_id_type=MESH).start()
        return carry

    lax.fori_loop(0, 16, send_fc2, 0)

    def wait_for(ref, sem):
        pltpu.make_async_copy(ref, ref, sem).wait()

    def denominator():
        wait_for(norms.at[pl.ds(0, 127)], norm_sem)
        total = jnp.sum(jnp.sum(norms[...], axis=0), axis=1, keepdims=True)
        return jnp.sqrt(total) + NORM_EPS

    @pl.when(is_own1)
    def _():
        partner = to(midx, 2 * xpos + 1 - core)
        norms[flat] = part1[midx]
        raw1[xpos * 16 + midx] = send1[midx]
        den = denominator()

        def push(slot, half):
            return pltpu.make_async_remote_copy(
                y_own.at[slot, :, pl.ds(half * 256, 256)], y_oth.at[slot, :, pl.ds(half * 256, 256)],
                y_send.at[slot, half], y_recv.at[slot, half], device_id=partner, device_id_type=MESH)

        def push_gram(slot):
            return pltpu.make_async_remote_copy(
                a_own.at[slot], a_oth.at[slot], a_send.at[slot], a_recv.at[slot],
                device_id=partner, device_id_type=MESH)

        for half in range(2):
            @pl.when(xpos // 2 == half)
            def _():
                wait_for(raw1.at[pl.ds(0, 31)], gather_sem.at[half])

            @pl.when(xpos // 2 != half)
            def _():
                wait_for(raw1.at[pl.ds(0, 32)], gather_sem.at[half])

            def scale(k, carry):
                for lane in (2 * half, 2 * half + 1):
                    block = raw1[lane * 16 + k].astype(F32) / den
                    y_own[0, pl.ds(k * 64, 64), lane * 128:(lane + 1) * 128] = block.astype(BF16)
                return carry

            lax.fori_loop(0, 16, scale, 0)
            push(0, half).start()

        def step(k, carry):
            now = k % 2
            nxt = 1 - now
            a_own[now] = dot(y_own[now], y_own[now], TN).astype(BF16)
            push_gram(now).start()
            for half in range(2):
                push(now, half).wait()
            a_cross[...] = dot(y_oth[now], y_own[now], TN).astype(BF16)
            own_sq = dot(a_own[now], a_own[now], NN) + dot(a_cross[...], a_cross[...], TN)
            b_own[...] = (NS_COEF_B * a_own[now].astype(F32) + NS_COEF_C * own_sq).astype(BF16)
            push_gram(now).wait()
            cross_sq = dot(a_cross[...], a_own[now], NN) + dot(a_oth[now], a_cross[...], NN)
            b_cross[...] = (NS_COEF_B * a_cross[...].astype(F32) + NS_COEF_C * cross_sq).astype(BF16)
            for half in range(2):
                lanes = slice(half * 256, (half + 1) * 256)
                update = dot(y_own[now], b_own[:, lanes], NN) + dot(y_oth[now], b_cross[:, lanes], NN)
                y_own[nxt, :, lanes] = (NS_COEF_A * y_own[now, :, lanes].astype(F32) + update).astype(BF16)

                @pl.when(k < NS_STEPS - 1)
                def _():
                    push(nxt, half).start()

                @pl.when(k == NS_STEPS - 1)
                def _():
                    def scatter(i, carry):
                        mm = (midx + i) % 16
                        for lane in (2 * half, 2 * half + 1):
                            @pl.when(jnp.logical_not(jnp.logical_and(mm == midx, lane == xpos)))
                            def _():
                                pltpu.make_async_remote_copy(
                                    y_own.at[nxt, pl.ds(mm * 64, 64), pl.ds(lane * 128, 128)], res1.at[midx],
                                    out_send, result_sem.at[0],
                                    device_id=to(mm, 2 * lane + core), device_id_type=MESH).start()
                        return carry
                    lax.fori_loop(0, 16, scatter, 0)
            return carry

        lax.fori_loop(0, NS_STEPS, step, 0)
        for lane in range(4):
            @pl.when(xpos == lane)
            def _():
                res1[midx] = y_own[NS_STEPS % 2, pl.ds(midx * 64, 64), lane * 128:(lane + 1) * 128]
        wait_for(raw1.at[pl.ds(0, 63)], out_send)
        wait_for(send1.at[pl.ds(0, 15)], send_sem.at[0])
        wait_for(norms.at[pl.ds(0, 31)], send_sem.at[1])
        wait_for(res1.at[pl.ds(0, 15)], result_sem.at[0])

    @pl.when(jnp.logical_not(is_own1))
    def _():
        wait_for(send1, send_sem.at[0])
        wait_for(norms.at[pl.ds(0, 32)], send_sem.at[1])

    @pl.when(is_own2)
    def _():
        norms[flat] = part2[midx]
        raw2[flat] = send2[midx]
        den = denominator()
        wait_for(raw2.at[pl.ds(0, 127)], gather_sem.at[0])

        def scale(k, carry):
            for d in range(8):
                block = raw2[k * 8 + d].astype(F32) / den
                y2[pl.ds(k * 32, 32), d * 128:(d + 1) * 128] = block.astype(BF16)
            return carry

        lax.fori_loop(0, 16, scale, 0)

        def step(k, carry):
            a2[...] = dot(y2[...], y2[...], NT).astype(BF16)
            b2[...] = (NS_COEF_B * a2[...].astype(F32) + NS_COEF_C * dot(a2[...], a2[...], NN)).astype(BF16)
            y2[...] = (NS_COEF_A * y2[...].astype(F32) + dot(b2[...], y2[...], NN)).astype(BF16)
            return carry

        lax.fori_loop(0, NS_STEPS, step, 0)

        def scatter(i, carry):
            mm = (midx + i) % 16
            for d in range(8):
                @pl.when(jnp.logical_not(jnp.logical_and(mm == midx, didx == d)))
                def _():
                    pltpu.make_async_remote_copy(
                        y2.at[pl.ds(mm * 32, 32), pl.ds(d * 128, 128)], res2.at[midx], out_send, result_sem.at[1],
                        device_id=to(mm, d), device_id_type=MESH).start()
            return carry

        lax.fori_loop(0, 16, scatter, 0)
        for d in range(8):
            @pl.when(didx == d)
            def _():
                res2[midx] = y2[pl.ds(midx * 32, 32), d * 128:(d + 1) * 128]
        wait_for(raw2.at[pl.ds(0, 127)], out_send)
        wait_for(send2.at[pl.ds(0, 15)], send_sem.at[2])
        wait_for(norms.at[pl.ds(0, 15)], send_sem.at[3])
        wait_for(res2.at[pl.ds(0, 15)], result_sem.at[1])

    @pl.when(jnp.logical_not(is_own2))
    def _():
        wait_for(send2, send_sem.at[2])
        wait_for(norms.at[pl.ds(0, 16)], send_sem.at[3])
        wait_for(res2, result_sem.at[1])

    @pl.when(jnp.logical_not(is_own1))
    def _():
        wait_for(res1, result_sem.at[0])


def exchange(m1, g1, m2, g2):
    hbm_spec = pl.BlockSpec(memory_space=pltpu.HBM)
    vmem_spec = pl.BlockSpec(memory_space=pltpu.VMEM)
    vmem = pltpu.VMEM
    sem = pltpu.SemaphoreType.DMA
    return pl.pallas_call(
        muon_kernel,
        out_shape=(jax.ShapeDtypeStruct((16, 64, 128), BF16), jax.ShapeDtypeStruct((16, 32, 128), BF16)),
        in_specs=[hbm_spec] * 4,
        out_specs=(vmem_spec, vmem_spec),
        scratch_shapes=[
            vmem((16, 64, 128), F32), vmem((16, 64, 128), BF16), vmem((16, 32, 128), F32), vmem((16, 32, 128), BF16),
            vmem((16, 64, 128), BF16), vmem((16, 32, 128), BF16), vmem((16, 1, 128), F32), vmem((16, 1, 128), F32),
            vmem((64, 64, 128), BF16), vmem((128, 32, 128), BF16), vmem((128, 1, 128), F32),
            vmem((2, 1024, 512), BF16), vmem((2, 1024, 512), BF16),
            vmem((2, 512, 512), BF16), vmem((512, 512), BF16), vmem((2, 512, 512), BF16),
            vmem((512, 512), BF16), vmem((512, 512), BF16),
            vmem((512, 1024), BF16), vmem((512, 512), BF16), vmem((512, 512), BF16),
            sem((4,)), sem((4,)), sem((2,)), sem, sem((2,)), sem((2, 2)), sem((2, 2)), sem((2,)), sem((2,)), sem,
        ],
        compiler_params=pltpu.CompilerParams(collective_id=0, has_side_effects=True, vmem_limit_bytes=48 << 20),
        name='muon_exchange',
    )(m1, g1, m2, g2)


def weight_step(weights, momentum, gradient, ortho_t, rows, cols):
    new_mom = MOMENTUM * momentum + gradient.astype(F32)
    ortho = jnp.swapaxes(ortho_t, 1, 2).astype(F32) * (0.2 * math.sqrt(max(rows, cols)))
    return weights - LEARN_RATE * (ortho + DECAY * weights), new_mom


def solution(mesh):
    block_spec = P('stage', 'data', 'model')

    def local_step(w1, m1, g1, w2, m2, g2):
        flip = functools.partial(jnp.swapaxes, axis1=1, axis2=2)
        ortho1, ortho2 = exchange(flip(m1), flip(g1), flip(m2), flip(g2))
        new_w1, new_m1 = weight_step(w1, m1, g1, ortho1, 1024, 1024)
        new_w2, new_m2 = weight_step(w2, m2, g2, ortho2, 1024, 512)
        return new_w1, new_m1, new_w2, new_m2

    return jax.shard_map(local_step, mesh=mesh, in_specs=(block_spec,) * 6, out_specs=(block_spec,) * 4, check_vma=False)
```

```python
import functools
import math
import jax
import jax.numpy as jnp
from jax import lax
from jax.experimental import pallas as pl
from jax.experimental.pallas import tpu as pltpu
from jax.sharding import PartitionSpec as P

NS_STEPS = 5
NS_COEF_A = 3.4445
NS_COEF_B = -4.7750
NS_COEF_C = 2.0315
MOMENTUM = 0.95
LEARN_RATE = 0.04
DECAY = 0.2
NORM_EPS = 1e-7

BF16 = jnp.bfloat16
F32 = jnp.float32
NN = ((1,), (0,))
TN = ((0,), (0,))
NT = ((1,), (1,))
MESH = pl.DeviceIdType.MESH


def dot(lhs, rhs, dims):
    return lax.dot_general(lhs, rhs, (dims, ((), ())), preferred_element_type=F32)


def muon_kernel(m1_hbm, g1_hbm, m2_hbm, g2_hbm, res1, res2,
                m1, g1, m2, g2, send1, send2, part1, part2,
                raw1, raw2, norms, y_own, y_oth, a_own, a_cross, a_oth, b_own, b_cross, square, y2, a2, b2,
                in_sem, send_sem, gather_sem, norm_sem, result_sem, y_send, y_recv, a_send, a_recv, out_send):
    midx = lax.axis_index('model')
    didx = lax.axis_index('data')
    core = didx % 2
    xpos = didx // 2
    diag = midx // 4 + midx % 4
    flat = midx * 8 + didx
    is_own1 = (8 - diag) % 4 == xpos
    is_own2 = jnp.logical_and((10 - diag) % 4 == xpos, core == 1)

    def to(model, data):
        return {'model': model, 'data': data}

    loads = [pltpu.make_async_copy(src, dst, in_sem.at[i])
             for i, (src, dst) in enumerate(((m1_hbm, m1), (g1_hbm, g1), (m2_hbm, m2), (g2_hbm, g2)))]
    for load in loads:
        load.start()

    barrier = pltpu.get_barrier_semaphore()

    def greet(i, carry):
        other = (flat + i) % 128
        pl.semaphore_signal(barrier, inc=1, device_id=to(other // 8, other % 8), device_id_type=MESH)
        return carry

    is_owner = jnp.logical_or(is_own1, is_own2)

    @pl.when(is_owner)
    def _():
        lax.fori_loop(1, 128, greet, 0)

    def momentum(e, carry, m_ref, g_ref, send, part):
        value = MOMENTUM * m_ref[e] + g_ref[e].astype(F32)
        send[e] = value.astype(BF16)
        part[e] = jnp.sum(value * value, axis=0, keepdims=True)
        return carry

    loads[0].wait()
    loads[1].wait()
    lax.fori_loop(0, 16, functools.partial(momentum, m_ref=m1, g_ref=g1, send=send1, part=part1), 0)
    loads[2].wait()
    loads[3].wait()
    lax.fori_loop(0, 16, functools.partial(momentum, m_ref=m2, g_ref=g2, send=send2, part=part2), 0)

    @pl.when(is_owner)
    def _():
        pl.semaphore_wait(barrier, 47)

    @pl.when(jnp.logical_not(is_owner))
    def _():
        pl.semaphore_wait(barrier, 48)

    def send_fc1(i, carry):
        e = (midx + 2 * didx + i) % 16
        ox = (8 - e // 4 - e % 4) % 4
        mine = jnp.logical_and(e == midx, is_own1)
        for side in range(2):
            @pl.when(jnp.logical_not(jnp.logical_and(mine, core == side)))
            def _():
                pltpu.make_async_remote_copy(
                    part1.at[e], norms.at[flat], send_sem.at[1], norm_sem,
                    device_id=to(e, 2 * ox + side), device_id_type=MESH).start()

        @pl.when(jnp.logical_not(mine))
        def _():
            pltpu.make_async_remote_copy(
                send1.at[e], raw1.at[midx * 4 + xpos], send_sem.at[0], gather_sem.at[midx // 4],
                device_id=to(e, 2 * ox + core), device_id_type=MESH).start()
        return carry

    lax.fori_loop(0, 16, send_fc1, 0)

    def send_fc2(i, carry):
        e = (midx + 2 * didx + i) % 16
        ox = (10 - e // 4 - e % 4) % 4

        @pl.when(jnp.logical_not(jnp.logical_and(e == midx, is_own2)))
        def _():
            pltpu.make_async_remote_copy(
                part2.at[e], norms.at[flat], send_sem.at[3], norm_sem,
                device_id=to(e, 2 * ox + 1), device_id_type=MESH).start()
            pltpu.make_async_remote_copy(
                send2.at[e], raw2.at[flat], send_sem.at[2], gather_sem.at[0],
                device_id=to(e, 2 * ox + 1), device_id_type=MESH).start()
        return carry

    lax.fori_loop(0, 16, send_fc2, 0)

    def wait_for(ref, sem):
        pltpu.make_async_copy(ref, ref, sem).wait()

    def denominator():
        wait_for(norms.at[pl.ds(0, 127)], norm_sem)
        total = jnp.sum(jnp.sum(norms[...], axis=0), axis=1, keepdims=True)
        return jnp.sqrt(total) + NORM_EPS

    @pl.when(is_own1)
    def _():
        partner = to(midx, 2 * xpos + 1 - core)
        norms[flat] = part1[midx]
        raw1[midx * 4 + xpos] = send1[midx]
        den = denominator()

        def push(slot, q):
            rows = (slot, pl.ds(q * 256, 256))
            return pltpu.make_async_remote_copy(
                y_own.at[rows], y_oth.at[rows], y_send.at[slot, q], y_recv.at[slot, q],
                device_id=partner, device_id_type=MESH)

        def push_gram(slot):
            return pltpu.make_async_remote_copy(
                a_own.at[slot], a_oth.at[slot], a_send.at[slot], a_recv.at[slot],
                device_id=partner, device_id_type=MESH)

        for q in range(4):
            @pl.when(midx // 4 == q)
            def _():
                wait_for(raw1.at[pl.ds(0, 15)], gather_sem.at[q])

            @pl.when(midx // 4 != q)
            def _():
                wait_for(raw1.at[pl.ds(0, 16)], gather_sem.at[q])

            def scale(k, carry):
                for lane in range(4):
                    block = raw1[k * 4 + lane].astype(F32) / den
                    y_own[0, pl.ds(k * 64, 64), lane * 128:(lane + 1) * 128] = block.astype(BF16)
                return carry

            lax.fori_loop(4 * q, 4 * q + 4, scale, 0)
            push(0, q).start()

        def scatter(slot, q):
            def body(i, carry):
                mm = 4 * q + (midx + i) % 4
                for lane in range(4):
                    @pl.when(jnp.logical_not(jnp.logical_and(mm == midx, lane == xpos)))
                    def _():
                        pltpu.make_async_remote_copy(
                            y_own.at[slot, pl.ds(mm * 64, 64), pl.ds(lane * 128, 128)], res1.at[midx],
                            out_send, result_sem.at[0],
                            device_id=to(mm, 2 * lane + core), device_id_type=MESH).start()
                return carry
            lax.fori_loop(0, 4, body, 0)

        def step(now, last):
            nxt = 1 - now
            a_own[now] = dot(y_own[now], y_own[now], TN).astype(BF16)
            push_gram(now).start()
            square[...] = dot(a_own[now], a_own[now], NN)
            cross = 0
            for q in range(4):
                push(now, q).wait()
                rows = slice(q * 256, (q + 1) * 256)
                cross = cross + dot(y_oth[now, rows], y_own[now, rows], TN)
            a_cross[...] = cross.astype(BF16)
            total = square[...] + dot(a_cross[...], a_cross[...], TN)
            b_own[...] = (NS_COEF_B * a_own[now].astype(F32) + NS_COEF_C * total).astype(BF16)
            square[...] = dot(a_cross[...], a_own[now], NN)
            push_gram(now).wait()
            total = square[...] + dot(a_oth[now], a_cross[...], NN)
            b_cross[...] = (NS_COEF_B * a_cross[...].astype(F32) + NS_COEF_C * total).astype(BF16)
            for q in range(4):
                rows = slice(q * 256, (q + 1) * 256)
                update = dot(y_own[now, rows], b_own[...], NN) + dot(y_oth[now, rows], b_cross[...], NN)
                y_own[nxt, rows] = (NS_COEF_A * y_own[now, rows].astype(F32) + update).astype(BF16)
                if last:
                    scatter(nxt, q)
                else:
                    push(nxt, q).start()

        def two_steps(k, carry):
            step(0, False)
            step(1, False)
            return carry

        lax.fori_loop(0, NS_STEPS // 2, two_steps, 0)
        step(0, True)
        for lane in range(4):
            @pl.when(xpos == lane)
            def _():
                res1[midx] = y_own[NS_STEPS % 2, pl.ds(midx * 64, 64), lane * 128:(lane + 1) * 128]
        wait_for(raw1.at[pl.ds(0, 63)], out_send)
        wait_for(send1.at[pl.ds(0, 15)], send_sem.at[0])
        wait_for(norms.at[pl.ds(0, 31)], send_sem.at[1])
        wait_for(res1.at[pl.ds(0, 15)], result_sem.at[0])

    @pl.when(jnp.logical_not(is_own1))
    def _():
        wait_for(send1, send_sem.at[0])
        wait_for(norms.at[pl.ds(0, 32)], send_sem.at[1])

    @pl.when(is_own2)
    def _():
        norms[flat] = part2[midx]
        raw2[flat] = send2[midx]
        den = denominator()
        wait_for(raw2.at[pl.ds(0, 127)], gather_sem.at[0])

        def scale(k, carry):
            for d in range(8):
                block = raw2[k * 8 + d].astype(F32) / den
                y2[pl.ds(k * 32, 32), d * 128:(d + 1) * 128] = block.astype(BF16)
            return carry

        lax.fori_loop(0, 16, scale, 0)

        def step(k, carry):
            a2[...] = dot(y2[...], y2[...], NT).astype(BF16)
            b2[...] = (NS_COEF_B * a2[...].astype(F32) + NS_COEF_C * dot(a2[...], a2[...], NN)).astype(BF16)
            y2[...] = (NS_COEF_A * y2[...].astype(F32) + dot(b2[...], y2[...], NN)).astype(BF16)
            return carry

        lax.fori_loop(0, NS_STEPS, step, 0)

        def scatter(i, carry):
            mm = (midx + i) % 16
            for d in range(8):
                @pl.when(jnp.logical_not(jnp.logical_and(mm == midx, didx == d)))
                def _():
                    pltpu.make_async_remote_copy(
                        y2.at[pl.ds(mm * 32, 32), pl.ds(d * 128, 128)], res2.at[midx], out_send, result_sem.at[1],
                        device_id=to(mm, d), device_id_type=MESH).start()
            return carry

        lax.fori_loop(0, 16, scatter, 0)
        for d in range(8):
            @pl.when(didx == d)
            def _():
                res2[midx] = y2[pl.ds(midx * 32, 32), d * 128:(d + 1) * 128]
        wait_for(raw2.at[pl.ds(0, 127)], out_send)
        wait_for(send2.at[pl.ds(0, 15)], send_sem.at[2])
        wait_for(norms.at[pl.ds(0, 15)], send_sem.at[3])
        wait_for(res2.at[pl.ds(0, 15)], result_sem.at[1])

    @pl.when(jnp.logical_not(is_own2))
    def _():
        wait_for(send2, send_sem.at[2])
        wait_for(norms.at[pl.ds(0, 16)], send_sem.at[3])
        wait_for(res2, result_sem.at[1])

    @pl.when(jnp.logical_not(is_own1))
    def _():
        wait_for(res1, result_sem.at[0])


def exchange(m1, g1, m2, g2):
    hbm_spec = pl.BlockSpec(memory_space=pltpu.HBM)
    vmem_spec = pl.BlockSpec(memory_space=pltpu.VMEM)
    vmem = pltpu.VMEM
    sem = pltpu.SemaphoreType.DMA
    return pl.pallas_call(
        muon_kernel,
        out_shape=(jax.ShapeDtypeStruct((16, 64, 128), BF16), jax.ShapeDtypeStruct((16, 32, 128), BF16)),
        in_specs=[hbm_spec] * 4,
        out_specs=(vmem_spec, vmem_spec),
        scratch_shapes=[
            vmem((16, 64, 128), F32), vmem((16, 64, 128), BF16), vmem((16, 32, 128), F32), vmem((16, 32, 128), BF16),
            vmem((16, 64, 128), BF16), vmem((16, 32, 128), BF16), vmem((16, 1, 128), F32), vmem((16, 1, 128), F32),
            vmem((64, 64, 128), BF16), vmem((128, 32, 128), BF16), vmem((128, 1, 128), F32),
            vmem((2, 1024, 512), BF16), vmem((2, 1024, 512), BF16),
            vmem((2, 512, 512), BF16), vmem((512, 512), BF16), vmem((2, 512, 512), BF16),
            vmem((512, 512), BF16), vmem((512, 512), BF16), vmem((512, 512), F32),
            vmem((512, 1024), BF16), vmem((512, 512), BF16), vmem((512, 512), BF16),
            sem((4,)), sem((4,)), sem((4,)), sem, sem((2,)), sem((2, 4)), sem((2, 4)), sem((2,)), sem((2,)), sem,
        ],
        compiler_params=pltpu.CompilerParams(collective_id=0, has_side_effects=True, vmem_limit_bytes=67043328),
        name='muon_exchange',
    )(m1, g1, m2, g2)


def weight_step(weights, momentum, gradient, ortho_t, rows, cols):
    new_mom = MOMENTUM * momentum + gradient.astype(F32)
    ortho = jnp.swapaxes(ortho_t, 1, 2).astype(F32) * (0.2 * math.sqrt(max(rows, cols)))
    return weights - LEARN_RATE * (ortho + DECAY * weights), new_mom


def solution(mesh):
    block_spec = P('stage', 'data', 'model')

    def local_step(w1, m1, g1, w2, m2, g2):
        flip = functools.partial(jnp.swapaxes, axis1=1, axis2=2)
        ortho1, ortho2 = exchange(flip(m1), flip(g1), flip(m2), flip(g2))
        new_w1, new_m1 = weight_step(w1, m1, g1, ortho1, 1024, 1024)
        new_w2, new_m2 = weight_step(w2, m2, g2, ortho2, 1024, 512)
        return new_w1, new_m1, new_w2, new_m2

    return jax.shard_map(local_step, mesh=mesh, in_specs=(block_spec,) * 6, out_specs=(block_spec,) * 4, check_vma=False)
```

```python
import functools
import math
import jax
import jax.numpy as jnp
from jax import lax
from jax.experimental import pallas as pl
from jax.experimental.pallas import tpu as pltpu
from jax.sharding import PartitionSpec as P

NS_STEPS = 5
NS_COEF_A = 3.4445
NS_COEF_B = -4.7750
NS_COEF_C = 2.0315
MOMENTUM = 0.95
LEARN_RATE = 0.04
DECAY = 0.2
NORM_EPS = 1e-7

BF16 = jnp.bfloat16
F32 = jnp.float32
NN = ((1,), (0,))
TN = ((0,), (0,))
NT = ((1,), (1,))
MESH = pl.DeviceIdType.MESH
SCALE = 0.2 * math.sqrt(1024)


def dot(lhs, rhs, dims):
    return lax.dot_general(lhs, rhs, (dims, ((), ())), preferred_element_type=F32)


def muon_kernel(m1_hbm, g1_hbm, m2_hbm, g2_hbm, w1_hbm, w2_hbm, new_w1, new_m1, new_w2, new_m2,
                m1, g1, m2, g2, w1, w2, res1, res2, send1, send2, part1, part2,
                raw1, raw2, norms, half_norm, y_own, y_oth, a_own, a_cross, a_oth, b_own, b_cross, square, y2, a2, b2,
                in_sem, send_sem, gather_sem, norm_sem, result_sem, y_send, y_recv, a_send, a_recv, out_send):
    midx = lax.axis_index('model')
    didx = lax.axis_index('data')
    core = didx % 2
    xpos = didx // 2
    diag = midx // 4 + midx % 4
    flat = midx * 8 + didx
    is_own1 = (8 - diag) % 4 == xpos
    is_own2 = jnp.logical_and((10 - diag) % 4 == xpos, core == 1)

    def to(model, data):
        return {'model': model, 'data': data}

    loads = [pltpu.make_async_copy(src, dst, in_sem.at[i])
             for i, (src, dst) in enumerate((
                 (m1_hbm, m1), (g1_hbm, g1), (m2_hbm, m2), (g2_hbm, g2), (w1_hbm, w1), (w2_hbm, w2)))]
    for load in loads[:4]:
        load.start()

    barrier = pltpu.get_barrier_semaphore()

    def greet(i, carry):
        other = (flat + i) % 128
        pl.semaphore_signal(barrier, inc=1, device_id=to(other // 8, other % 8), device_id_type=MESH)
        return carry

    @pl.when(is_own1)
    def _():
        def greet_side(i, carry):
            other = (flat + 2 * i) % 128
            pl.semaphore_signal(barrier, inc=1, device_id=to(other // 8, other % 8), device_id_type=MESH)
            return carry

        lax.fori_loop(1, 64, greet_side, 0)
        pl.semaphore_signal(barrier, inc=1, device_id=to(midx, 2 * xpos + 1 - core), device_id_type=MESH)

    @pl.when(is_own2)
    def _():
        lax.fori_loop(1, 128, greet, 0)

    def momentum(e, carry, m_ref, g_ref, new_m, send, part):
        value = MOMENTUM * m_ref[e] + g_ref[e].astype(F32)
        new_m[e] = value
        send[e] = value.astype(BF16)
        part[e] = jnp.sum(value * value, axis=0, keepdims=True)
        return carry

    loads[0].wait()
    loads[1].wait()
    lax.fori_loop(0, 16, functools.partial(momentum, m_ref=m1, g_ref=g1, new_m=new_m1, send=send1, part=part1), 0)
    loads[2].wait()
    loads[3].wait()
    lax.fori_loop(0, 16, functools.partial(momentum, m_ref=m2, g_ref=g2, new_m=new_m2, send=send2, part=part2), 0)

    @pl.when(is_own2)
    def _():
        pl.semaphore_wait(barrier, 31)

    @pl.when(jnp.logical_not(is_own2))
    def _():
        pl.semaphore_wait(barrier, 32)

    def owner_fc1(i):
        e = (midx + 2 * didx + i) % 16
        ox = (8 - e // 4 - e % 4) % 4
        return e, jnp.logical_not(jnp.logical_and(e == midx, is_own1)), to(e, 2 * ox + core)

    def send_norm1(i, carry):
        e, away, owner = owner_fc1(i)

        @pl.when(away)
        def _():
            pltpu.make_async_remote_copy(
                part1.at[e], norms.at[midx * 4 + xpos], send_sem.at[1], norm_sem.at[0],
                device_id=owner, device_id_type=MESH).start()
        return carry

    lax.fori_loop(0, 16, send_norm1, 0)

    def send_fc1(i, carry):
        e, away, owner = owner_fc1(i)

        @pl.when(away)
        def _():
            pltpu.make_async_remote_copy(
                send1.at[e], raw1.at[midx * 4 + xpos], send_sem.at[0], gather_sem.at[midx // 4],
                device_id=owner, device_id_type=MESH).start()
        return carry

    lax.fori_loop(0, 16, send_fc1, 0)

    def send_fc2(i, carry):
        e = (midx + 2 * didx + i) % 16
        ox = (10 - e // 4 - e % 4) % 4

        @pl.when(jnp.logical_not(jnp.logical_and(e == midx, is_own2)))
        def _():
            pltpu.make_async_remote_copy(
                part2.at[e], norms.at[flat], send_sem.at[3], norm_sem.at[0],
                device_id=to(e, 2 * ox + 1), device_id_type=MESH).start()
            pltpu.make_async_remote_copy(
                send2.at[e], raw2.at[flat], send_sem.at[2], gather_sem.at[0],
                device_id=to(e, 2 * ox + 1), device_id_type=MESH).start()
        return carry

    lax.fori_loop(0, 16, send_fc2, 0)
    for load in loads[4:]:
        load.start()

    def wait_for(ref, sem):
        pltpu.make_async_copy(ref, ref, sem).wait()

    def inverse_norm(total):
        return 1.0 / (jnp.sqrt(jnp.sum(total, axis=1, keepdims=True)) + NORM_EPS)

    @pl.when(is_own1)
    def _():
        partner = to(midx, 2 * xpos + 1 - core)
        norms[midx * 4 + xpos] = part1[midx]
        raw1[midx * 4 + xpos] = send1[midx]
        wait_for(norms.at[pl.ds(0, 63)], norm_sem.at[0])
        half_norm[0] = jnp.sum(norms[:64], axis=0)
        swap = pltpu.make_async_remote_copy(
            half_norm.at[0], half_norm.at[1], norm_sem.at[1], norm_sem.at[2], device_id=partner, device_id_type=MESH)
        swap.start()
        swap.wait()
        inv = inverse_norm(half_norm[0] + half_norm[1])

        def push(slot, q):
            rows = (slot, pl.ds(q * 256, 256))
            return pltpu.make_async_remote_copy(
                y_own.at[rows], y_oth.at[rows], y_send.at[slot, q], y_recv.at[slot, q],
                device_id=partner, device_id_type=MESH)

        def push_gram(slot):
            return pltpu.make_async_remote_copy(
                a_own.at[slot], a_oth.at[slot], a_send.at[slot], a_recv.at[slot],
                device_id=partner, device_id_type=MESH)

        for q in range(4):
            @pl.when(midx // 4 == q)
            def _():
                wait_for(raw1.at[pl.ds(0, 15)], gather_sem.at[q])

            @pl.when(midx // 4 != q)
            def _():
                wait_for(raw1.at[pl.ds(0, 16)], gather_sem.at[q])

            def scale(k, carry):
                for lane in range(4):
                    block = raw1[k * 4 + lane].astype(F32) * inv
                    y_own[0, pl.ds(k * 64, 64), lane * 128:(lane + 1) * 128] = block.astype(BF16)
                return carry

            lax.fori_loop(4 * q, 4 * q + 4, scale, 0)
            push(0, q).start()

        def scatter(slot, q):
            def body(i, carry):
                mm = 4 * q + (midx + i) % 4
                for lane in range(4):
                    @pl.when(jnp.logical_not(jnp.logical_and(mm == midx, lane == xpos)))
                    def _():
                        pltpu.make_async_remote_copy(
                            y_own.at[slot, pl.ds(mm * 64, 64), pl.ds(lane * 128, 128)], res1.at[midx],
                            out_send, result_sem.at[0],
                            device_id=to(mm, 2 * lane + core), device_id_type=MESH).start()
                return carry
            lax.fori_loop(0, 4, body, 0)

        def step(now, last):
            nxt = 1 - now
            a_own[now] = dot(y_own[now], y_own[now], TN).astype(BF16)
            push_gram(now).start()
            square[...] = dot(a_own[now], a_own[now], NN)
            cross = 0
            for q in range(4):
                push(now, q).wait()
                rows = slice(q * 256, (q + 1) * 256)
                cross = cross + dot(y_oth[now, rows], y_own[now, rows], TN)
            a_cross[...] = cross.astype(BF16)
            total = square[...] + dot(a_cross[...], a_cross[...], TN)
            b_own[...] = (NS_COEF_B * a_own[now].astype(F32) + NS_COEF_C * total).astype(BF16)
            square[...] = dot(a_cross[...], a_own[now], NN)
            push_gram(now).wait()
            total = square[...] + dot(a_oth[now], a_cross[...], NN)
            b_cross[...] = (NS_COEF_B * a_cross[...].astype(F32) + NS_COEF_C * total).astype(BF16)
            for q in range(4):
                rows = slice(q * 256, (q + 1) * 256)
                update = dot(y_own[now, rows], b_own[...], NN) + dot(y_oth[now, rows], b_cross[...], NN)
                y_own[nxt, rows] = (NS_COEF_A * y_own[now, rows].astype(F32) + update).astype(BF16)
                if last:
                    scatter(nxt, q)
                else:
                    push(nxt, q).start()

        def two_steps(k, carry):
            step(0, False)
            step(1, False)
            return carry

        lax.fori_loop(0, NS_STEPS // 2, two_steps, 0)
        step(0, True)
        for lane in range(4):
            @pl.when(xpos == lane)
            def _():
                res1[midx] = y_own[NS_STEPS % 2, pl.ds(midx * 64, 64), lane * 128:(lane + 1) * 128]
        wait_for(raw1.at[pl.ds(0, 63)], out_send)
        wait_for(send1.at[pl.ds(0, 15)], send_sem.at[0])
        wait_for(norms.at[pl.ds(0, 15)], send_sem.at[1])

    @pl.when(jnp.logical_not(is_own1))
    def _():
        wait_for(send1, send_sem.at[0])
        wait_for(norms.at[pl.ds(0, 16)], send_sem.at[1])

    @pl.when(is_own2)
    def _():
        norms[flat] = part2[midx]
        raw2[flat] = send2[midx]
        wait_for(norms.at[pl.ds(0, 127)], norm_sem.at[0])
        inv = inverse_norm(jnp.sum(norms[...], axis=0))
        wait_for(raw2.at[pl.ds(0, 127)], gather_sem.at[0])

        def scale(k, carry):
            for d in range(8):
                block = raw2[k * 8 + d].astype(F32) * inv
                y2[pl.ds(k * 32, 32), d * 128:(d + 1) * 128] = block.astype(BF16)
            return carry

        lax.fori_loop(0, 16, scale, 0)

        def step(k, carry):
            a2[...] = dot(y2[...], y2[...], NT).astype(BF16)
            b2[...] = (NS_COEF_B * a2[...].astype(F32) + NS_COEF_C * dot(a2[...], a2[...], NN)).astype(BF16)
            y2[...] = (NS_COEF_A * y2[...].astype(F32) + dot(b2[...], y2[...], NN)).astype(BF16)
            return carry

        lax.fori_loop(0, NS_STEPS, step, 0)

        def scatter(i, carry):
            mm = (midx + i) % 16
            for d in range(8):
                @pl.when(jnp.logical_not(jnp.logical_and(mm == midx, didx == d)))
                def _():
                    pltpu.make_async_remote_copy(
                        y2.at[pl.ds(mm * 32, 32), pl.ds(d * 128, 128)], res2.at[midx], out_send, result_sem.at[1],
                        device_id=to(mm, d), device_id_type=MESH).start()
            return carry

        lax.fori_loop(0, 16, scatter, 0)
        for d in range(8):
            @pl.when(didx == d)
            def _():
                res2[midx] = y2[pl.ds(midx * 32, 32), d * 128:(d + 1) * 128]
        wait_for(raw2.at[pl.ds(0, 127)], out_send)
        wait_for(send2.at[pl.ds(0, 15)], send_sem.at[2])
        wait_for(norms.at[pl.ds(0, 15)], send_sem.at[3])

    @pl.when(jnp.logical_not(is_own2))
    def _():
        wait_for(send2, send_sem.at[2])
        wait_for(norms.at[pl.ds(0, 16)], send_sem.at[3])

    def weight_step(e, carry, w_ref, res, new_w, scale):
        old = w_ref[e]
        new_w[e] = old - LEARN_RATE * (res[e].astype(F32) * scale + DECAY * old)
        return carry

    for index, mine, res, w_ref, new_w, scale in (
            (1, is_own2, res2, w2, new_w2, SCALE), (0, is_own1, res1, w1, new_w1, SCALE)):
        @pl.when(mine)
        def _():
            wait_for(res.at[pl.ds(0, 15)], result_sem.at[index])

        @pl.when(jnp.logical_not(mine))
        def _():
            wait_for(res, result_sem.at[index])

        loads[5 if index else 4].wait()
        lax.fori_loop(0, 16, functools.partial(weight_step, w_ref=w_ref, res=res, new_w=new_w, scale=scale), 0)


def store_kernel(*refs):
    sem = refs[8]
    copies = [pltpu.make_async_copy(refs[i], refs[4 + i], sem.at[i]) for i in range(4)]
    for copy in copies:
        copy.start()
    for copy in copies:
        copy.wait()


def local_update(w1, m1, g1, w2, m2, g2):
    hbm_spec = pl.BlockSpec(memory_space=pltpu.HBM)
    vmem_spec = pl.BlockSpec(memory_space=pltpu.VMEM)
    vmem = pltpu.VMEM
    sem = pltpu.SemaphoreType.DMA
    big, small = (16, 64, 128), (16, 32, 128)
    outs = tuple(jax.ShapeDtypeStruct(shape, F32) for shape in (big, big, small, small))
    operands = (pltpu.with_memory_space_constraint(x, pltpu.HBM) for x in (m1, g1, m2, g2, w1, w2))
    updated = pl.pallas_call(
        muon_kernel,
        out_shape=outs,
        in_specs=[hbm_spec] * 6,
        out_specs=(vmem_spec,) * 4,
        scratch_shapes=[
            vmem(big, F32), vmem(big, BF16), vmem(small, F32), vmem(small, BF16), vmem(big, F32), vmem(small, F32),
            vmem(big, BF16), vmem(small, BF16),
            vmem(big, BF16), vmem(small, BF16), vmem((16, 1, 128), F32), vmem((16, 1, 128), F32),
            vmem((64, 64, 128), BF16), vmem((128, 32, 128), BF16), vmem((128, 1, 128), F32), vmem((2, 1, 128), F32),
            vmem((2, 1024, 512), BF16), vmem((2, 1024, 512), BF16),
            vmem((2, 512, 512), BF16), vmem((512, 512), BF16), vmem((2, 512, 512), BF16),
            vmem((512, 512), BF16), vmem((512, 512), BF16), vmem((512, 512), F32),
            vmem((512, 1024), BF16), vmem((512, 512), BF16), vmem((512, 512), BF16),
            sem((6,)), sem((4,)), sem((4,)), sem((3,)), sem((2,)), sem((2, 4)), sem((2, 4)), sem((2,)), sem((2,)), sem,
        ],
        compiler_params=pltpu.CompilerParams(collective_id=0, has_side_effects=True, vmem_limit_bytes=40 << 20),
        name='muon_exchange',
    )(*operands)
    return pl.pallas_call(
        store_kernel,
        out_shape=outs,
        in_specs=[vmem_spec] * 4,
        out_specs=(hbm_spec,) * 4,
        scratch_shapes=[sem((4,))],
        name='store_outputs',
    )(*(pltpu.with_memory_space_constraint(x, pltpu.VMEM) for x in updated))


def solution(mesh):
    block_spec = P('stage', 'data', 'model')

    def local_step(*args):
        return tuple(jnp.swapaxes(out, 1, 2) for out in local_update(*(jnp.swapaxes(arg, 1, 2) for arg in args)))

    return jax.shard_map(local_step, mesh=mesh, in_specs=(block_spec,) * 6, out_specs=(block_spec,) * 4, check_vma=False)
```

```python
import functools
import math
import jax
import jax.numpy as jnp
from jax import lax
from jax.experimental import pallas as pl
from jax.experimental.pallas import tpu as pltpu
from jax.sharding import PartitionSpec as P

NS_STEPS = 5
NS_COEF_A = 3.4445
NS_COEF_B = -4.7750
NS_COEF_C = 2.0315
MOMENTUM = 0.95
LEARN_RATE = 0.04
DECAY = 0.2
NORM_EPS = 1e-7

BF16 = jnp.bfloat16
F32 = jnp.float32
NN = ((1,), (0,))
TN = ((0,), (0,))
NT = ((1,), (1,))
MESH = pl.DeviceIdType.MESH
SCALE = 0.2 * math.sqrt(1024)


def dot(lhs, rhs, dims):
    return lax.dot_general(lhs, rhs, (dims, ((), ())), preferred_element_type=F32)


def muon_kernel(m1_hbm, g1_hbm, m2_hbm, g2_hbm, w1_hbm, w2_hbm, new_w1, new_m1, new_w2, new_m2,
                m1, g1, m2, g2, w1, w2, res1, res2, send1, send2, part1, part2,
                raw1, raw2, norms, half_norm, relay, y_own, y_oth, a_own, a_cross, a_oth, b_own, b_cross, square, y2, a2, b2,
                in_sem, send_sem, gather_sem, norm_sem, relay_sem, result_sem, y_send, y_recv, a_send, a_recv, out_send):
    midx = lax.axis_index('model')
    didx = lax.axis_index('data')
    core = didx % 2
    xpos = didx // 2
    diag = midx // 4 + midx % 4
    flat = midx * 8 + didx
    is_own1 = (8 - diag) % 4 == xpos
    is_own2 = jnp.logical_and((10 - diag) % 4 == xpos, core == 1)

    def to(model, data):
        return {'model': model, 'data': data}

    loads = [pltpu.make_async_copy(src, dst, in_sem.at[i])
             for i, (src, dst) in enumerate((
                 (m1_hbm, m1), (g1_hbm, g1), (m2_hbm, m2), (g2_hbm, g2), (w1_hbm, w1), (w2_hbm, w2)))]
    for load in loads[:4]:
        load.start()

    barrier = pltpu.get_barrier_semaphore()

    def greet(i, carry):
        other = (flat + i) % 128
        pl.semaphore_signal(barrier, inc=1, device_id=to(other // 8, other % 8), device_id_type=MESH)
        return carry

    @pl.when(is_own1)
    def _():
        def greet_side(i, carry):
            other = (flat + 2 * i) % 128
            pl.semaphore_signal(barrier, inc=1, device_id=to(other // 8, other % 8), device_id_type=MESH)
            return carry

        lax.fori_loop(1, 64, greet_side, 0)
        pl.semaphore_signal(barrier, inc=1, device_id=to(midx, 2 * xpos + 1 - core), device_id_type=MESH)

    @pl.when(is_own2)
    def _():
        lax.fori_loop(1, 128, greet, 0)

    def momentum(e, carry, m_ref, g_ref, new_m, send, part):
        value = MOMENTUM * m_ref[e] + g_ref[e].astype(F32)
        new_m[e] = value
        send[e] = value.astype(BF16)
        part[e] = jnp.sum(value * value, axis=0, keepdims=True)
        return carry

    loads[0].wait()
    loads[1].wait()
    lax.fori_loop(0, 16, functools.partial(momentum, m_ref=m1, g_ref=g1, new_m=new_m1, send=send1, part=part1), 0, unroll=True)

    @pl.when(is_own2)
    def _():
        pl.semaphore_wait(barrier, 31)

    @pl.when(jnp.logical_not(is_own2))
    def _():
        pl.semaphore_wait(barrier, 32)

    def owner_fc1(i):
        e = (midx + 2 * didx + i) % 16
        ox = (8 - e // 4 - e % 4) % 4
        return e, jnp.logical_not(jnp.logical_and(e == midx, is_own1)), to(e, 2 * ox + core)

    def send_norm1(i, carry):
        e, away, owner = owner_fc1(i)

        @pl.when(away)
        def _():
            pltpu.make_async_remote_copy(
                part1.at[e], norms.at[midx * 4 + xpos], send_sem.at[1], norm_sem.at[0],
                device_id=owner, device_id_type=MESH).start()
        return carry

    lax.fori_loop(0, 16, send_norm1, 0, unroll=True)

    def send_fc1(i, carry):
        e, away, owner = owner_fc1(i)

        @pl.when(away)
        def _():
            pltpu.make_async_remote_copy(
                send1.at[e], raw1.at[midx * 4 + xpos], send_sem.at[0], gather_sem.at[midx // 4],
                device_id=owner, device_id_type=MESH).start()
        return carry

    lax.fori_loop(0, 16, send_fc1, 0, unroll=True)

    loads[2].wait()
    loads[3].wait()
    lax.fori_loop(0, 16, functools.partial(momentum, m_ref=m2, g_ref=g2, new_m=new_m2, send=send2, part=part2), 0)

    def send_fc2(i, carry):
        e = (midx + 2 * didx + i) % 16
        ox = (10 - e // 4 - e % 4) % 4

        @pl.when(jnp.logical_not(jnp.logical_and(e == midx, is_own2)))
        def _():
            pltpu.make_async_remote_copy(
                part2.at[e], norms.at[flat], send_sem.at[3], norm_sem.at[0],
                device_id=to(e, 2 * ox + 1), device_id_type=MESH).start()
            pltpu.make_async_remote_copy(
                send2.at[e], raw2.at[flat], send_sem.at[2], gather_sem.at[0],
                device_id=to(e, 2 * ox + 1), device_id_type=MESH).start()
        return carry

    lax.fori_loop(0, 16, send_fc2, 0)
    for load in loads[4:]:
        load.start()

    def wait_for(ref, sem):
        pltpu.make_async_copy(ref, ref, sem).wait()

    def inverse_norm(total):
        return 1.0 / (jnp.sqrt(jnp.sum(total, axis=1, keepdims=True)) + NORM_EPS)

    @pl.when(is_own1)
    def _():
        partner = to(midx, 2 * xpos + 1 - core)
        norms[midx * 4 + xpos] = part1[midx]
        raw1[midx * 4 + xpos] = send1[midx]
        wait_for(norms.at[pl.ds(0, 63)], norm_sem.at[0])
        half_norm[0] = jnp.sum(norms[:64], axis=0)
        swap = pltpu.make_async_remote_copy(
            half_norm.at[0], half_norm.at[1], norm_sem.at[1], norm_sem.at[2], device_id=partner, device_id_type=MESH)
        swap.start()
        swap.wait()
        inv = inverse_norm(half_norm[0] + half_norm[1])

        def push(slot, q):
            rows = (slot, pl.ds(q * 256, 256))
            return pltpu.make_async_remote_copy(
                y_own.at[rows], y_oth.at[rows], y_send.at[slot, q], y_recv.at[slot, q],
                device_id=partner, device_id_type=MESH)

        def push_gram(slot):
            return pltpu.make_async_remote_copy(
                a_own.at[slot], a_oth.at[slot], a_send.at[slot], a_recv.at[slot],
                device_id=partner, device_id_type=MESH)

        for q in range(4):
            @pl.when(midx // 4 == q)
            def _():
                wait_for(raw1.at[pl.ds(0, 15)], gather_sem.at[q])

            @pl.when(midx // 4 != q)
            def _():
                wait_for(raw1.at[pl.ds(0, 16)], gather_sem.at[q])

            def scale(k, carry):
                for lane in range(4):
                    block = raw1[k * 4 + lane].astype(F32) * inv
                    y_own[0, pl.ds(k * 64, 64), lane * 128:(lane + 1) * 128] = block.astype(BF16)
                return carry

            lax.fori_loop(4 * q, 4 * q + 4, scale, 0, unroll=True)
            push(0, q).start()

        def scatter(slot, q):
            def body(i, carry):
                mm = 4 * q + (midx + i) % 4
                rows = (slot, pl.ds(mm * 64, 64))
                far = pl.multiple_of((xpos + 2) % 4 * 128, 128)

                @pl.when(mm != midx)
                def _():
                    pltpu.make_async_remote_copy(
                        y_own.at[(*rows, pl.ds(far, 128))], relay.at[midx // 4], out_send, relay_sem.at[midx // 4],
                        device_id=to(mm, 2 * xpos + core), device_id_type=MESH).start()

                for hop in (1, 3, 0, 2):
                    lane = (xpos + hop) % 4
                    direct = {0: mm != midx, 2: mm == midx}.get(hop)

                    def send():
                        pltpu.make_async_remote_copy(
                            y_own.at[(*rows, pl.ds(pl.multiple_of(lane * 128, 128), 128))], res1.at[midx],
                            out_send, result_sem.at[0],
                            device_id=to(mm, 2 * lane + core), device_id_type=MESH).start()

                    if direct is None:
                        send()
                    else:
                        pl.when(direct)(send)
                return carry
            lax.fori_loop(0, 4, body, 0, unroll=True)

        def step(now, last):
            nxt = 1 - now
            a_own[now] = dot(y_own[now], y_own[now], TN).astype(BF16)
            push_gram(now).start()
            square[...] = dot(a_own[now], a_own[now], NN)
            cross = 0
            for q in range(4):
                push(now, q).wait()
                rows = slice(q * 256, (q + 1) * 256)
                cross = cross + dot(y_oth[now, rows], y_own[now, rows], TN)
            a_cross[...] = cross.astype(BF16)
            total = square[...] + dot(a_cross[...], a_cross[...], TN)
            b_own[...] = (NS_COEF_B * a_own[now].astype(F32) + NS_COEF_C * total).astype(BF16)
            square[...] = dot(a_cross[...], a_own[now], NN)
            push_gram(now).wait()
            total = square[...] + dot(a_oth[now], a_cross[...], NN)
            b_cross[...] = (NS_COEF_B * a_cross[...].astype(F32) + NS_COEF_C * total).astype(BF16)
            for q in range(4):
                rows = slice(q * 256, (q + 1) * 256)
                update = dot(y_own[now, rows], b_own[...], NN) + dot(y_oth[now, rows], b_cross[...], NN)
                y_own[nxt, rows] = (NS_COEF_A * y_own[now, rows].astype(F32) + update).astype(BF16)
                if last:
                    scatter(nxt, q)
                else:
                    push(nxt, q).start()

        def two_steps(k, carry):
            step(0, False)
            step(1, False)
            return carry

        lax.fori_loop(0, NS_STEPS // 2, two_steps, 0)
        step(0, True)
        for lane in range(4):
            @pl.when(xpos == lane)
            def _():
                res1[midx] = y_own[NS_STEPS % 2, pl.ds(midx * 64, 64), lane * 128:(lane + 1) * 128]
        wait_for(raw1.at[pl.ds(0, 63)], out_send)
        wait_for(send1.at[pl.ds(0, 15)], send_sem.at[0])
        wait_for(norms.at[pl.ds(0, 15)], send_sem.at[1])

    @pl.when(jnp.logical_not(is_own1))
    def _():
        wait_for(send1, send_sem.at[0])
        wait_for(norms.at[pl.ds(0, 16)], send_sem.at[1])

    @pl.when(is_own2)
    def _():
        norms[flat] = part2[midx]
        raw2[flat] = send2[midx]
        wait_for(norms.at[pl.ds(0, 127)], norm_sem.at[0])
        inv = inverse_norm(jnp.sum(norms[...], axis=0))
        wait_for(raw2.at[pl.ds(0, 127)], gather_sem.at[0])

        def scale(k, carry):
            for d in range(8):
                block = raw2[k * 8 + d].astype(F32) * inv
                y2[pl.ds(k * 32, 32), d * 128:(d + 1) * 128] = block.astype(BF16)
            return carry

        lax.fori_loop(0, 16, scale, 0)

        def step(k, carry):
            a2[...] = dot(y2[...], y2[...], NT).astype(BF16)
            b2[...] = (NS_COEF_B * a2[...].astype(F32) + NS_COEF_C * dot(a2[...], a2[...], NN)).astype(BF16)
            y2[...] = (NS_COEF_A * y2[...].astype(F32) + dot(b2[...], y2[...], NN)).astype(BF16)
            return carry

        lax.fori_loop(0, NS_STEPS, step, 0)

        def scatter(i, carry):
            mm = (midx + i) % 16
            for d in range(8):
                @pl.when(jnp.logical_not(jnp.logical_and(mm == midx, didx == d)))
                def _():
                    pltpu.make_async_remote_copy(
                        y2.at[pl.ds(mm * 32, 32), pl.ds(d * 128, 128)], res2.at[midx], out_send, result_sem.at[1],
                        device_id=to(mm, d), device_id_type=MESH).start()
            return carry

        lax.fori_loop(0, 16, scatter, 0)
        for d in range(8):
            @pl.when(didx == d)
            def _():
                res2[midx] = y2[pl.ds(midx * 32, 32), d * 128:(d + 1) * 128]
        wait_for(raw2.at[pl.ds(0, 127)], out_send)
        wait_for(send2.at[pl.ds(0, 15)], send_sem.at[2])
        wait_for(norms.at[pl.ds(0, 15)], send_sem.at[3])

    @pl.when(jnp.logical_not(is_own2))
    def _():
        wait_for(send2, send_sem.at[2])
        wait_for(norms.at[pl.ds(0, 16)], send_sem.at[3])

    def weight_step(e, carry, w_ref, res, new_w, scale):
        old = w_ref[e]
        new_w[e] = old - LEARN_RATE * (res[e].astype(F32) * scale + DECAY * old)
        return carry

    def finish(index, mine, res, w_ref, new_w):
        @pl.when(mine)
        def _():
            wait_for(res.at[pl.ds(0, 15)], result_sem.at[index])

        @pl.when(jnp.logical_not(mine))
        def _():
            wait_for(res, result_sem.at[index])

        loads[4 + index].wait()
        lax.fori_loop(0, 16, functools.partial(weight_step, w_ref=w_ref, res=res, new_w=new_w, scale=SCALE), 0, unroll=True)

    finish(1, is_own2, res2, w2, new_w2)

    def forward(j, carry):
        e = 4 * j + (8 - xpos - j) % 4

        @pl.when(e != midx)
        def _():
            wait_for(relay.at[j], relay_sem.at[j])
            pltpu.make_async_remote_copy(
                relay.at[j], res1.at[e], relay_sem.at[4], result_sem.at[0],
                device_id=to(midx, 2 * ((xpos + 2) % 4) + core), device_id_type=MESH).start()
        return carry

    lax.fori_loop(0, 4, forward, 0)
    finish(0, is_own1, res1, w1, new_w1)

    @pl.when(is_own1)
    def _():
        wait_for(relay.at[pl.ds(0, 3)], relay_sem.at[4])

    @pl.when(jnp.logical_not(is_own1))
    def _():
        wait_for(relay, relay_sem.at[4])


def store_kernel(*refs):
    sem = refs[8]
    copies = [pltpu.make_async_copy(refs[i], refs[4 + i], sem.at[i]) for i in range(4)]
    for copy in copies:
        copy.start()
    for copy in copies:
        copy.wait()


def local_update(w1, m1, g1, w2, m2, g2):
    hbm_spec = pl.BlockSpec(memory_space=pltpu.HBM)
    vmem_spec = pl.BlockSpec(memory_space=pltpu.VMEM)
    vmem = pltpu.VMEM
    sem = pltpu.SemaphoreType.DMA
    big, small = (16, 64, 128), (16, 32, 128)
    outs = tuple(jax.ShapeDtypeStruct(shape, F32) for shape in (big, big, small, small))
    operands = (pltpu.with_memory_space_constraint(x, pltpu.HBM) for x in (m1, g1, m2, g2, w1, w2))
    updated = pl.pallas_call(
        muon_kernel,
        out_shape=outs,
        in_specs=[hbm_spec] * 6,
        out_specs=(vmem_spec,) * 4,
        scratch_shapes=[
            vmem(big, F32), vmem(big, BF16), vmem(small, F32), vmem(small, BF16), vmem(big, F32), vmem(small, F32),
            vmem(big, BF16), vmem(small, BF16),
            vmem(big, BF16), vmem(small, BF16), vmem((16, 1, 128), F32), vmem((16, 1, 128), F32),
            vmem((64, 64, 128), BF16), vmem((128, 32, 128), BF16), vmem((128, 1, 128), F32), vmem((2, 1, 128), F32), vmem((4, 64, 128), BF16),
            vmem((2, 1024, 512), BF16), vmem((2, 1024, 512), BF16),
            vmem((2, 512, 512), BF16), vmem((512, 512), BF16), vmem((2, 512, 512), BF16),
            vmem((512, 512), BF16), vmem((512, 512), BF16), vmem((512, 512), F32),
            vmem((512, 1024), BF16), vmem((512, 512), BF16), vmem((512, 512), BF16),
            sem((6,)), sem((4,)), sem((4,)), sem((3,)), sem((5,)), sem((2,)), sem((2, 4)), sem((2, 4)), sem((2,)), sem((2,)), sem,
        ],
        compiler_params=pltpu.CompilerParams(collective_id=0, has_side_effects=True, vmem_limit_bytes=40 << 20),
        name='muon_exchange',
    )(*operands)
    return pl.pallas_call(
        store_kernel,
        out_shape=outs,
        in_specs=[vmem_spec] * 4,
        out_specs=(hbm_spec,) * 4,
        scratch_shapes=[sem((4,))],
        name='store_outputs',
    )(*(pltpu.with_memory_space_constraint(x, pltpu.VMEM) for x in updated))


def solution(mesh):
    block_spec = P('stage', 'data', 'model')

    def local_step(*args):
        return tuple(jnp.swapaxes(out, 1, 2) for out in local_update(*(jnp.swapaxes(arg, 1, 2) for arg in args)))

    return jax.shard_map(local_step, mesh=mesh, in_specs=(block_spec,) * 6, out_specs=(block_spec,) * 4, check_vma=False)
```

```python
import functools
import math
import jax
import jax.numpy as jnp
from jax import lax
from jax.experimental import pallas as pl
from jax.experimental.pallas import tpu as pltpu
from jax.sharding import PartitionSpec as P

NS_STEPS = 5
NS_COEF_A = 3.4445
NS_COEF_B = -4.7750
NS_COEF_C = 2.0315
MOMENTUM = 0.95
LEARN_RATE = 0.04
DECAY = 0.2
NORM_EPS = 1e-7

BF16 = jnp.bfloat16
F32 = jnp.float32
NN = ((1,), (0,))
TN = ((0,), (0,))
NT = ((1,), (1,))
MESH = pl.DeviceIdType.MESH
SCALE = 0.2 * math.sqrt(1024)


def dot(lhs, rhs, dims):
    return lax.dot_general(lhs, rhs, (dims, ((), ())), preferred_element_type=F32)


def muon_kernel(m1_hbm, g1_hbm, m2_hbm, g2_hbm, w1_hbm, w2_hbm, new_w1, new_m1, new_w2, new_m2,
                m1, g1, m2, g2, w1, w2, res1, res2, send1, send2, part1, part2,
                raw1, raw2, norms, half_norm, relay, y_own, y_oth, a_own, a_cross, a_oth, b_own, b_cross, square, y2, a2, b2,
                in_sem, send_sem, gather_sem, norm_sem, relay_sem, result_sem, y_send, y_recv, a_send, a_recv, out_send):
    midx = lax.axis_index('model')
    didx = lax.axis_index('data')
    core = didx % 2
    xpos = didx // 2
    diag = midx // 4 + midx % 4
    flat = midx * 8 + didx
    is_own1 = (8 - diag) % 4 == xpos
    is_own2 = jnp.logical_and((10 - diag) % 4 == xpos, core == 1)

    def to(model, data):
        return {'model': model, 'data': data}

    loads = [pltpu.make_async_copy(src, dst, in_sem.at[i])
             for i, (src, dst) in enumerate((
                 (m1_hbm, m1), (g1_hbm, g1), (m2_hbm, m2), (g2_hbm, g2), (w1_hbm, w1), (w2_hbm, w2)))]
    for load in loads[:4]:
        load.start()

    def wait_for(ref, sem):
        pltpu.make_async_copy(ref, ref, sem).wait()

    barrier = pltpu.get_barrier_semaphore()

    def greet(i, carry):
        other = (flat + i) % 128
        pl.semaphore_signal(barrier, inc=1, device_id=to(other // 8, other % 8), device_id_type=MESH)
        return carry

    @pl.when(is_own1)
    def _():
        def greet_side(i, carry):
            other = (flat + 2 * i) % 128
            pl.semaphore_signal(barrier, inc=1, device_id=to(other // 8, other % 8), device_id_type=MESH)
            return carry

        lax.fori_loop(1, 64, greet_side, 0, unroll=True)
        pl.semaphore_signal(barrier, inc=1, device_id=to(midx, 2 * xpos + 1 - core), device_id_type=MESH)

    @pl.when(is_own2)
    def _():
        lax.fori_loop(1, 128, greet, 0, unroll=True)

    def momentum(e, carry, m_ref, g_ref, new_m, send, part):
        value = MOMENTUM * m_ref[e] + g_ref[e].astype(F32)
        new_m[e] = value
        send[e] = value.astype(BF16)
        part[e] = jnp.sum(value * value, axis=0, keepdims=True)
        return carry

    loads[0].wait()
    loads[1].wait()
    lax.fori_loop(0, 16, functools.partial(momentum, m_ref=m1, g_ref=g1, new_m=new_m1, send=send1, part=part1), 0, unroll=True)

    @pl.when(is_own2)
    def _():
        pl.semaphore_wait(barrier, 31)

    @pl.when(jnp.logical_not(is_own2))
    def _():
        pl.semaphore_wait(barrier, 32)

    def owner_fc1(i):
        hop = (2, 1, 3, 0)[i // 4]
        e = 4 * ((midx // 4 + hop) % 4) + (midx + didx + i) % 4
        ox = (8 - e // 4 - e % 4) % 4
        return e, jnp.logical_not(jnp.logical_and(e == midx, is_own1)), to(e, 2 * ox + core)

    def send_norm1(i, carry):
        e, away, owner = owner_fc1(i)

        @pl.when(away)
        def _():
            pltpu.make_async_remote_copy(
                part1.at[e], norms.at[midx * 4 + xpos], send_sem.at[1], norm_sem.at[0],
                device_id=owner, device_id_type=MESH).start()
        return carry

    for i in range(16):
        send_norm1(i, 0)

    def send_fc1(i, carry):
        e, away, owner = owner_fc1(i)

        @pl.when(away)
        def _():
            pltpu.make_async_remote_copy(
                send1.at[e], raw1.at[midx * 4 + xpos], send_sem.at[0], gather_sem.at[midx // 4],
                device_id=owner, device_id_type=MESH).start()
        return carry

    for i in range(16):
        send_fc1(i, 0)

    loads[2].wait()
    loads[3].wait()
    lax.fori_loop(0, 16, functools.partial(momentum, m_ref=m2, g_ref=g2, new_m=new_m2, send=send2, part=part2), 0)

    @pl.when(is_own1)
    def _():
        wait_for(send1.at[pl.ds(0, 15)], send_sem.at[0])

    @pl.when(jnp.logical_not(is_own1))
    def _():
        wait_for(send1, send_sem.at[0])

    def send_fc2(i, carry):
        e = (midx + 2 * didx + i) % 16
        ox = (10 - e // 4 - e % 4) % 4

        @pl.when(jnp.logical_not(jnp.logical_and(e == midx, is_own2)))
        def _():
            pltpu.make_async_remote_copy(
                part2.at[e], norms.at[flat], send_sem.at[3], norm_sem.at[0],
                device_id=to(e, 2 * ox + 1), device_id_type=MESH).start()
            pltpu.make_async_remote_copy(
                send2.at[e], raw2.at[flat], send_sem.at[2], gather_sem.at[0],
                device_id=to(e, 2 * ox + 1), device_id_type=MESH).start()
        return carry

    lax.fori_loop(0, 16, send_fc2, 0)
    for load in loads[4:]:
        load.start()

    def inverse_norm(total):
        return 1.0 / (jnp.sqrt(jnp.sum(total, axis=1, keepdims=True)) + NORM_EPS)

    @pl.when(is_own1)
    def _():
        partner = to(midx, 2 * xpos + 1 - core)
        norms[midx * 4 + xpos] = part1[midx]
        raw1[midx * 4 + xpos] = send1[midx]
        wait_for(norms.at[pl.ds(0, 63)], norm_sem.at[0])
        half_norm[0] = jnp.sum(norms[:64], axis=0)
        swap = pltpu.make_async_remote_copy(
            half_norm.at[0], half_norm.at[1], norm_sem.at[1], norm_sem.at[2], device_id=partner, device_id_type=MESH)
        swap.start()
        swap.wait()
        inv = inverse_norm(half_norm[0] + half_norm[1])

        def push(slot, q):
            rows = (slot, pl.ds(pl.multiple_of(q * 256, 256), 256))
            return pltpu.make_async_remote_copy(
                y_own.at[rows], y_oth.at[rows], y_send.at[slot, q], y_recv.at[slot, q],
                device_id=partner, device_id_type=MESH)

        def push_gram(slot):
            return pltpu.make_async_remote_copy(
                a_own.at[slot], a_oth.at[slot], a_send.at[slot], a_recv.at[slot],
                device_id=partner, device_id_type=MESH)

        for hop in (0, 1, 3, 2):
            q = (midx // 4 + hop) % 4
            wait_for(raw1.at[pl.ds(0, 15 if hop == 0 else 16)], gather_sem.at[q])

            def scale(k, carry):
                for lane in range(4):
                    block = raw1[k * 4 + lane].astype(F32) * inv
                    y_own[0, pl.ds(pl.multiple_of(k * 64, 64), 64), lane * 128:(lane + 1) * 128] = block.astype(BF16)
                return carry

            for k in range(4):
                scale(4 * q + k, 0)
            push(0, q).start()
            rows = pl.ds(pl.multiple_of(q * 256, 256), 256)
            part = dot(y_own[0, rows], y_own[0, rows], TN)
            square[...] = part if hop == 0 else square[...] + part

        def scatter(slot, q):
            def body(i, carry):
                mm = 4 * q + (midx + i) % 4
                rows = (slot, pl.ds(mm * 64, 64))
                far = pl.multiple_of((xpos + 2) % 4 * 128, 128)

                @pl.when(mm != midx)
                def _():
                    pltpu.make_async_remote_copy(
                        y_own.at[(*rows, pl.ds(far, 128))], relay.at[midx // 4], out_send, relay_sem.at[midx // 4],
                        device_id=to(mm, 2 * xpos + core), device_id_type=MESH).start()

                for hop in (1, 3, 0, 2):
                    lane = (xpos + hop) % 4
                    direct = {0: mm != midx, 2: mm == midx}.get(hop)

                    def send():
                        pltpu.make_async_remote_copy(
                            y_own.at[(*rows, pl.ds(pl.multiple_of(lane * 128, 128), 128))], res1.at[midx],
                            out_send, result_sem.at[0],
                            device_id=to(mm, 2 * lane + core), device_id_type=MESH).start()

                    if direct is None:
                        send()
                    else:
                        pl.when(direct)(send)
                return carry
            lax.fori_loop(0, 4, body, 0, unroll=True)

        def gram(slot, value):
            a_own[slot] = value.astype(BF16)
            push_gram(slot).start()

        def step(now, last):
            nxt = 1 - now
            square[...] = dot(a_own[now], a_own[now], NN)
            cross = 0
            for q in range(4):
                push(now, q).wait()
                rows = slice(q * 256, (q + 1) * 256)
                cross = cross + dot(y_oth[now, rows], y_own[now, rows], TN)
            a_cross[...] = cross.astype(BF16)
            total = square[...] + dot(a_cross[...], a_cross[...], TN)
            b_own[...] = (NS_COEF_B * a_own[now].astype(F32) + NS_COEF_C * total).astype(BF16)
            square[...] = dot(a_cross[...], a_own[now], NN)
            push_gram(now).wait()
            total = square[...] + dot(a_oth[now], a_cross[...], NN)
            b_cross[...] = (NS_COEF_B * a_cross[...].astype(F32) + NS_COEF_C * total).astype(BF16)
            for q in range(4):
                rows = slice(q * 256, (q + 1) * 256)
                update = dot(y_own[now, rows], b_own[...], NN) + dot(y_oth[now, rows], b_cross[...], NN)
                y_own[nxt, rows] = (NS_COEF_A * y_own[now, rows].astype(F32) + update).astype(BF16)
                if last:
                    scatter(nxt, q)
                else:
                    push(nxt, q).start()
            if not last:
                gram(nxt, dot(y_own[nxt], y_own[nxt], TN))

        gram(0, square[...])

        def two_steps(k, carry):
            step(0, False)
            step(1, False)
            return carry

        lax.fori_loop(0, NS_STEPS // 2, two_steps, 0)
        step(0, True)
        for lane in range(4):
            @pl.when(xpos == lane)
            def _():
                res1[midx] = y_own[NS_STEPS % 2, pl.ds(midx * 64, 64), lane * 128:(lane + 1) * 128]
        wait_for(norms.at[pl.ds(0, 15)], send_sem.at[1])

    @pl.when(jnp.logical_not(is_own1))
    def _():
        wait_for(norms.at[pl.ds(0, 16)], send_sem.at[1])

    @pl.when(is_own2)
    def _():
        norms[flat] = part2[midx]
        raw2[flat] = send2[midx]
        wait_for(norms.at[pl.ds(0, 127)], norm_sem.at[0])
        inv = inverse_norm(jnp.sum(norms[...], axis=0))
        wait_for(raw2.at[pl.ds(0, 127)], gather_sem.at[0])

        def scale(k, carry):
            for d in range(8):
                block = raw2[k * 8 + d].astype(F32) * inv
                y2[pl.ds(k * 32, 32), d * 128:(d + 1) * 128] = block.astype(BF16)
            return carry

        lax.fori_loop(0, 16, scale, 0)

        def step(k, carry):
            a2[...] = dot(y2[...], y2[...], NT).astype(BF16)
            b2[...] = (NS_COEF_B * a2[...].astype(F32) + NS_COEF_C * dot(a2[...], a2[...], NN)).astype(BF16)
            y2[...] = (NS_COEF_A * y2[...].astype(F32) + dot(b2[...], y2[...], NN)).astype(BF16)
            return carry

        lax.fori_loop(0, NS_STEPS, step, 0)

        def scatter(i, carry):
            mm = (midx + i) % 16
            for d in range(8):
                @pl.when(jnp.logical_not(jnp.logical_and(mm == midx, didx == d)))
                def _():
                    pltpu.make_async_remote_copy(
                        y2.at[pl.ds(mm * 32, 32), pl.ds(d * 128, 128)], res2.at[midx], out_send, result_sem.at[1],
                        device_id=to(mm, d), device_id_type=MESH).start()
            return carry

        lax.fori_loop(0, 16, scatter, 0)
        for d in range(8):
            @pl.when(didx == d)
            def _():
                res2[midx] = y2[pl.ds(midx * 32, 32), d * 128:(d + 1) * 128]
        wait_for(raw2.at[pl.ds(0, 127)], out_send)
        wait_for(send2.at[pl.ds(0, 15)], send_sem.at[2])
        wait_for(norms.at[pl.ds(0, 15)], send_sem.at[3])

    @pl.when(jnp.logical_not(is_own2))
    def _():
        wait_for(send2, send_sem.at[2])
        wait_for(norms.at[pl.ds(0, 16)], send_sem.at[3])

    def weight_step(e, carry, w_ref, res, new_w, scale):
        old = w_ref[e]
        new_w[e] = old - LEARN_RATE * (res[e].astype(F32) * scale + DECAY * old)
        return carry

    def finish(index, mine, res, w_ref, new_w):
        @pl.when(mine)
        def _():
            wait_for(res.at[pl.ds(0, 15)], result_sem.at[index])

        @pl.when(jnp.logical_not(mine))
        def _():
            wait_for(res, result_sem.at[index])

        loads[4 + index].wait()
        lax.fori_loop(0, 16, functools.partial(weight_step, w_ref=w_ref, res=res, new_w=new_w, scale=SCALE), 0, unroll=True)

    finish(1, is_own2, res2, w2, new_w2)

    def forward(j, carry):
        e = 4 * j + (8 - xpos - j) % 4

        @pl.when(e != midx)
        def _():
            wait_for(relay.at[j], relay_sem.at[j])
            pltpu.make_async_remote_copy(
                relay.at[j], res1.at[e], relay_sem.at[4], result_sem.at[0],
                device_id=to(midx, 2 * ((xpos + 2) % 4) + core), device_id_type=MESH).start()
        return carry

    lax.fori_loop(0, 4, forward, 0)
    finish(0, is_own1, res1, w1, new_w1)

    @pl.when(is_own1)
    def _():
        wait_for(raw1.at[pl.ds(0, 63)], out_send)
        wait_for(relay.at[pl.ds(0, 3)], relay_sem.at[4])

    @pl.when(jnp.logical_not(is_own1))
    def _():
        wait_for(relay, relay_sem.at[4])


def store_kernel(*refs):
    sem = refs[8]
    copies = [pltpu.make_async_copy(refs[i], refs[4 + i], sem.at[i]) for i in range(4)]
    for copy in copies:
        copy.start()
    for copy in copies:
        copy.wait()


def local_update(w1, m1, g1, w2, m2, g2):
    hbm_spec = pl.BlockSpec(memory_space=pltpu.HBM)
    vmem_spec = pl.BlockSpec(memory_space=pltpu.VMEM)
    vmem = pltpu.VMEM
    sem = pltpu.SemaphoreType.DMA
    big, small = (16, 64, 128), (16, 32, 128)
    outs = tuple(jax.ShapeDtypeStruct(shape, F32) for shape in (big, big, small, small))
    operands = (pltpu.with_memory_space_constraint(x, pltpu.HBM) for x in (m1, g1, m2, g2, w1, w2))
    updated = pl.pallas_call(
        muon_kernel,
        out_shape=outs,
        in_specs=[hbm_spec] * 6,
        out_specs=(vmem_spec,) * 4,
        scratch_shapes=[
            vmem(big, F32), vmem(big, BF16), vmem(small, F32), vmem(small, BF16), vmem(big, F32), vmem(small, F32),
            vmem(big, BF16), vmem(small, BF16),
            vmem(big, BF16), vmem(small, BF16), vmem((16, 1, 128), F32), vmem((16, 1, 128), F32),
            vmem((64, 64, 128), BF16), vmem((128, 32, 128), BF16), vmem((128, 1, 128), F32), vmem((2, 1, 128), F32), vmem((4, 64, 128), BF16),
            vmem((2, 1024, 512), BF16), vmem((2, 1024, 512), BF16),
            vmem((2, 512, 512), BF16), vmem((512, 512), BF16), vmem((2, 512, 512), BF16),
            vmem((512, 512), BF16), vmem((512, 512), BF16), vmem((512, 512), F32),
            vmem((512, 1024), BF16), vmem((512, 512), BF16), vmem((512, 512), BF16),
            sem((6,)), sem((4,)), sem((4,)), sem((3,)), sem((5,)), sem((2,)), sem((2, 4)), sem((2, 4)), sem((2,)), sem((2,)), sem,
        ],
        compiler_params=pltpu.CompilerParams(collective_id=0, has_side_effects=True, vmem_limit_bytes=40 << 20),
        name='muon_exchange',
    )(*operands)
    return pl.pallas_call(
        store_kernel,
        out_shape=outs,
        in_specs=[vmem_spec] * 4,
        out_specs=(hbm_spec,) * 4,
        scratch_shapes=[sem((4,))],
        name='store_outputs',
    )(*(pltpu.with_memory_space_constraint(x, pltpu.VMEM) for x in updated))


def solution(mesh):
    block_spec = P('stage', 'data', 'model')

    def local_step(*args):
        return tuple(jnp.swapaxes(out, 1, 2) for out in local_update(*(jnp.swapaxes(arg, 1, 2) for arg in args)))

    return jax.shard_map(local_step, mesh=mesh, in_specs=(block_spec,) * 6, out_specs=(block_spec,) * 4, check_vma=False)
```

```python
import functools
import math
import jax
import jax.numpy as jnp
from jax import lax
from jax.experimental import pallas as pl
from jax.experimental.pallas import tpu as pltpu
from jax.sharding import PartitionSpec as P

NS_STEPS = 5
NS_COEF_A = 3.4445
NS_COEF_B = -4.7750
NS_COEF_C = 2.0315
MOMENTUM = 0.95
LEARN_RATE = 0.04
DECAY = 0.2
NORM_EPS = 1e-7

BF16 = jnp.bfloat16
F32 = jnp.float32
NN = ((1,), (0,))
TN = ((0,), (0,))
NT = ((1,), (1,))
MESH = pl.DeviceIdType.MESH
SCALE = 0.2 * math.sqrt(1024)


def dot(lhs, rhs, dims):
    return lax.dot_general(lhs, rhs, (dims, ((), ())), preferred_element_type=F32)


def muon_kernel(m1_hbm, g1_hbm, m2_hbm, g2_hbm, w1_hbm, w2_hbm, new_w1, new_m1, new_w2, new_m2,
                m1, g1, m2, g2, w1, w2, res1, res2, send1, send2, part1, part2,
                raw1, raw2, norms, half_norm, relay, y_own, y_oth, a_own, a_cross, a_oth, b_own, b_cross, square, y2, a2, b2,
                in_sem, send_sem, gather_sem, norm_sem, relay_sem, result_sem, y_send, y_recv, a_send, a_recv, out_send):
    midx = lax.axis_index('model')
    didx = lax.axis_index('data')
    core = didx % 2
    xpos = didx // 2
    diag = midx // 4 + midx % 4
    flat = midx * 8 + didx
    is_own1 = (8 - diag) % 4 == xpos
    is_own2 = jnp.logical_and((10 - diag) % 4 == xpos, core == 1)

    def to(model, data):
        return {'model': model, 'data': data}

    loads = [pltpu.make_async_copy(src, dst, in_sem.at[i])
             for i, (src, dst) in enumerate((
                 (m1_hbm, m1), (g1_hbm, g1), (m2_hbm, m2), (g2_hbm, g2), (w1_hbm, w1), (w2_hbm, w2)))]
    for load in loads[:4]:
        load.start()

    def wait_for(ref, sem):
        pltpu.make_async_copy(ref, ref, sem).wait()

    barrier = pltpu.get_barrier_semaphore()

    def greet(i, carry):
        other = (flat + i) % 128
        pl.semaphore_signal(barrier, inc=1, device_id=to(other // 8, other % 8), device_id_type=MESH)
        return carry

    @pl.when(is_own1)
    def _():
        def greet_side(i, carry):
            other = (flat + 2 * i) % 128
            pl.semaphore_signal(barrier, inc=1, device_id=to(other // 8, other % 8), device_id_type=MESH)
            return carry

        lax.fori_loop(1, 64, greet_side, 0, unroll=True)
        pl.semaphore_signal(barrier, inc=1, device_id=to(midx, 2 * xpos + 1 - core), device_id_type=MESH)

    @pl.when(is_own2)
    def _():
        lax.fori_loop(1, 128, greet, 0, unroll=True)

    def momentum(e, carry, m_ref, g_ref, new_m, send, part):
        value = MOMENTUM * m_ref[e] + g_ref[e].astype(F32)
        new_m[e] = value
        send[e] = value.astype(BF16)
        part[e] = jnp.sum(value * value, axis=0, keepdims=True)
        return carry

    loads[0].wait()
    loads[1].wait()
    lax.fori_loop(0, 16, functools.partial(momentum, m_ref=m1, g_ref=g1, new_m=new_m1, send=send1, part=part1), 0, unroll=True)

    @pl.when(is_own2)
    def _():
        pl.semaphore_wait(barrier, 31)

    @pl.when(jnp.logical_not(is_own2))
    def _():
        pl.semaphore_wait(barrier, 32)

    def owner_fc1(i):
        hop = (2, 1, 3, 0)[i // 4]
        e = 4 * ((midx // 4 + hop) % 4) + (midx + didx + i) % 4
        ox = (8 - e // 4 - e % 4) % 4
        return e, jnp.logical_not(jnp.logical_and(e == midx, is_own1)), to(e, 2 * ox + core)

    def send_norm1(i, carry):
        e, away, owner = owner_fc1(i)

        @pl.when(away)
        def _():
            pltpu.make_async_remote_copy(
                part1.at[e], norms.at[midx * 4 + xpos], send_sem.at[1], norm_sem.at[0],
                device_id=owner, device_id_type=MESH).start()
        return carry

    for i in range(16):
        send_norm1(i, 0)

    def send_fc1(i, carry):
        e, away, owner = owner_fc1(i)

        @pl.when(away)
        def _():
            pltpu.make_async_remote_copy(
                send1.at[e], raw1.at[midx * 4 + xpos], send_sem.at[0], gather_sem.at[midx // 4],
                device_id=owner, device_id_type=MESH).start()
        return carry

    for i in range(16):
        send_fc1(i, 0)

    loads[2].wait()
    loads[3].wait()
    lax.fori_loop(0, 16, functools.partial(momentum, m_ref=m2, g_ref=g2, new_m=new_m2, send=send2, part=part2), 0)

    @pl.when(is_own1)
    def _():
        wait_for(send1.at[pl.ds(0, 15)], send_sem.at[0])

    @pl.when(jnp.logical_not(is_own1))
    def _():
        wait_for(send1, send_sem.at[0])

    def send_fc2(i, carry):
        e = (midx + 2 * didx + i) % 16
        ox = (10 - e // 4 - e % 4) % 4

        @pl.when(jnp.logical_not(jnp.logical_and(e == midx, is_own2)))
        def _():
            pltpu.make_async_remote_copy(
                part2.at[e], norms.at[flat], send_sem.at[3], norm_sem.at[0],
                device_id=to(e, 2 * ox + 1), device_id_type=MESH).start()
            pltpu.make_async_remote_copy(
                send2.at[e], raw2.at[flat], send_sem.at[2], gather_sem.at[0],
                device_id=to(e, 2 * ox + 1), device_id_type=MESH).start()
        return carry

    lax.fori_loop(0, 16, send_fc2, 0)
    for load in loads[4:]:
        load.start()

    def inverse_norm(total):
        return 1.0 / (jnp.sqrt(jnp.sum(total, axis=1, keepdims=True)) + NORM_EPS)

    @pl.when(is_own1)
    def _():
        partner = to(midx, 2 * xpos + 1 - core)
        norms[midx * 4 + xpos] = part1[midx]
        raw1[midx * 4 + xpos] = send1[midx]
        wait_for(norms.at[pl.ds(0, 63)], norm_sem.at[0])
        half_norm[0] = jnp.sum(norms[:64], axis=0)
        swap = pltpu.make_async_remote_copy(
            half_norm.at[0], half_norm.at[1], norm_sem.at[1], norm_sem.at[2], device_id=partner, device_id_type=MESH)
        swap.start()
        swap.wait()
        inv = inverse_norm(half_norm[0] + half_norm[1])

        def push(slot, q):
            rows = (slot, pl.ds(pl.multiple_of(q * 256, 256), 256))
            return pltpu.make_async_remote_copy(
                y_own.at[rows], y_oth.at[rows], y_send.at[slot, q], y_recv.at[slot, q],
                device_id=partner, device_id_type=MESH)

        def push_gram(slot):
            return pltpu.make_async_remote_copy(
                a_own.at[slot], a_oth.at[slot], a_send.at[slot], a_recv.at[slot],
                device_id=partner, device_id_type=MESH)

        for hop in (0, 1, 3, 2):
            q = (midx // 4 + hop) % 4
            wait_for(raw1.at[pl.ds(0, 15 if hop == 0 else 16)], gather_sem.at[q])

            def scale(k, carry):
                for lane in range(4):
                    block = raw1[k * 4 + lane].astype(F32) * inv
                    y_own[0, pl.ds(pl.multiple_of(k * 64, 64), 64), lane * 128:(lane + 1) * 128] = block.astype(BF16)
                return carry

            for k in range(4):
                scale(4 * q + k, 0)
            push(0, q).start()
            rows = pl.ds(pl.multiple_of(q * 256, 256), 256)
            part = dot(y_own[0, rows], y_own[0, rows], TN)
            square[...] = part if hop == 0 else square[...] + part

        def scatter(slot, q):
            def place(i):
                mm = 4 * q + i
                return mm, (slot, pl.ds(mm * 64, 64))

            for i in range(4):
                mm, rows = place(i)
                far = pl.multiple_of((xpos + 2) % 4 * 128, 128)

                @pl.when(mm != midx)
                def _():
                    pltpu.make_async_remote_copy(
                        y_own.at[(*rows, pl.ds(far, 128))], relay.at[midx // 4], out_send, relay_sem.at[midx // 4],
                        device_id=to(mm, 2 * xpos + core), device_id_type=MESH).start()

            for i in range(4):
                mm, rows = place(i)
                for hop in (1, 3, 0, 2):
                    lane = (xpos + hop) % 4
                    direct = {0: mm != midx, 2: mm == midx}.get(hop)

                    def send():
                        pltpu.make_async_remote_copy(
                            y_own.at[(*rows, pl.ds(pl.multiple_of(lane * 128, 128), 128))], res1.at[midx],
                            out_send, result_sem.at[0],
                            device_id=to(mm, 2 * lane + core), device_id_type=MESH).start()

                    if direct is None:
                        send()
                    else:
                        pl.when(direct)(send)

        def gram(slot, value):
            a_own[slot] = value.astype(BF16)
            push_gram(slot).start()

        def step(now, last):
            nxt = 1 - now
            square[...] = dot(a_own[now], a_own[now], NN)
            cross = 0
            for q in range(4):
                push(now, q).wait()
                rows = slice(q * 256, (q + 1) * 256)
                cross = cross + dot(y_oth[now, rows], y_own[now, rows], TN)
            a_cross[...] = cross.astype(BF16)
            total = square[...] + dot(a_cross[...], a_cross[...], TN)
            b_own[...] = (NS_COEF_B * a_own[now].astype(F32) + NS_COEF_C * total).astype(BF16)
            square[...] = dot(a_cross[...], a_own[now], NN)
            push_gram(now).wait()
            total = square[...] + dot(a_oth[now], a_cross[...], NN)
            b_cross[...] = (NS_COEF_B * a_cross[...].astype(F32) + NS_COEF_C * total).astype(BF16)
            for q in range(4):
                rows = slice(q * 256, (q + 1) * 256)
                update = dot(y_own[now, rows], b_own[...], NN) + dot(y_oth[now, rows], b_cross[...], NN)
                y_own[nxt, rows] = (NS_COEF_A * y_own[now, rows].astype(F32) + update).astype(BF16)
                if last:
                    scatter(nxt, q)
                else:
                    push(nxt, q).start()
            if not last:
                gram(nxt, dot(y_own[nxt], y_own[nxt], TN))

        gram(0, square[...])

        def two_steps(k, carry):
            step(0, False)
            step(1, False)
            return carry

        lax.fori_loop(0, NS_STEPS // 2, two_steps, 0)
        step(0, True)
        for lane in range(4):
            @pl.when(xpos == lane)
            def _():
                res1[midx] = y_own[NS_STEPS % 2, pl.ds(midx * 64, 64), lane * 128:(lane + 1) * 128]
        wait_for(norms.at[pl.ds(0, 15)], send_sem.at[1])

    @pl.when(jnp.logical_not(is_own1))
    def _():
        wait_for(norms.at[pl.ds(0, 16)], send_sem.at[1])

    @pl.when(is_own2)
    def _():
        norms[flat] = part2[midx]
        raw2[flat] = send2[midx]
        wait_for(norms.at[pl.ds(0, 127)], norm_sem.at[0])
        inv = inverse_norm(jnp.sum(norms[...], axis=0))
        wait_for(raw2.at[pl.ds(0, 127)], gather_sem.at[0])

        def scale(k, carry):
            for d in range(8):
                block = raw2[k * 8 + d].astype(F32) * inv
                y2[pl.ds(k * 32, 32), d * 128:(d + 1) * 128] = block.astype(BF16)
            return carry

        lax.fori_loop(0, 16, scale, 0)

        def step(k, carry):
            a2[...] = dot(y2[...], y2[...], NT).astype(BF16)
            b2[...] = (NS_COEF_B * a2[...].astype(F32) + NS_COEF_C * dot(a2[...], a2[...], NN)).astype(BF16)
            y2[...] = (NS_COEF_A * y2[...].astype(F32) + dot(b2[...], y2[...], NN)).astype(BF16)
            return carry

        lax.fori_loop(0, NS_STEPS, step, 0)

        def scatter(i, carry):
            mm = (midx + i) % 16
            for d in range(8):
                @pl.when(jnp.logical_not(jnp.logical_and(mm == midx, didx == d)))
                def _():
                    pltpu.make_async_remote_copy(
                        y2.at[pl.ds(mm * 32, 32), pl.ds(d * 128, 128)], res2.at[midx], out_send, result_sem.at[1],
                        device_id=to(mm, d), device_id_type=MESH).start()
            return carry

        lax.fori_loop(0, 16, scatter, 0)
        for d in range(8):
            @pl.when(didx == d)
            def _():
                res2[midx] = y2[pl.ds(midx * 32, 32), d * 128:(d + 1) * 128]
        wait_for(raw2.at[pl.ds(0, 127)], out_send)
        wait_for(send2.at[pl.ds(0, 15)], send_sem.at[2])
        wait_for(norms.at[pl.ds(0, 15)], send_sem.at[3])

    @pl.when(jnp.logical_not(is_own2))
    def _():
        wait_for(send2, send_sem.at[2])
        wait_for(norms.at[pl.ds(0, 16)], send_sem.at[3])

    def weight_step(e, carry, w_ref, res, new_w, scale):
        old = w_ref[e]
        new_w[e] = old - LEARN_RATE * (res[e].astype(F32) * scale + DECAY * old)
        return carry

    def finish(index, mine, res, w_ref, new_w):
        @pl.when(mine)
        def _():
            wait_for(res.at[pl.ds(0, 15)], result_sem.at[index])

        @pl.when(jnp.logical_not(mine))
        def _():
            wait_for(res, result_sem.at[index])

        loads[4 + index].wait()
        lax.fori_loop(0, 16, functools.partial(weight_step, w_ref=w_ref, res=res, new_w=new_w, scale=SCALE), 0, unroll=True)

    finish(1, is_own2, res2, w2, new_w2)

    def forward(j, carry):
        e = 4 * j + (8 - xpos - j) % 4

        @pl.when(e != midx)
        def _():
            wait_for(relay.at[j], relay_sem.at[j])
            pltpu.make_async_remote_copy(
                relay.at[j], res1.at[e], relay_sem.at[4], result_sem.at[0],
                device_id=to(midx, 2 * ((xpos + 2) % 4) + core), device_id_type=MESH).start()
        return carry

    lax.fori_loop(0, 4, forward, 0)
    finish(0, is_own1, res1, w1, new_w1)

    @pl.when(is_own1)
    def _():
        wait_for(raw1.at[pl.ds(0, 63)], out_send)
        wait_for(relay.at[pl.ds(0, 3)], relay_sem.at[4])

    @pl.when(jnp.logical_not(is_own1))
    def _():
        wait_for(relay, relay_sem.at[4])


def store_kernel(*refs):
    sem = refs[8]
    copies = [pltpu.make_async_copy(refs[i], refs[4 + i], sem.at[i]) for i in range(4)]
    for copy in copies:
        copy.start()
    for copy in copies:
        copy.wait()


def local_update(w1, m1, g1, w2, m2, g2):
    hbm_spec = pl.BlockSpec(memory_space=pltpu.HBM)
    vmem_spec = pl.BlockSpec(memory_space=pltpu.VMEM)
    vmem = pltpu.VMEM
    sem = pltpu.SemaphoreType.DMA
    big, small = (16, 64, 128), (16, 32, 128)
    outs = tuple(jax.ShapeDtypeStruct(shape, F32) for shape in (big, big, small, small))
    operands = (pltpu.with_memory_space_constraint(x, pltpu.HBM) for x in (m1, g1, m2, g2, w1, w2))
    updated = pl.pallas_call(
        muon_kernel,
        out_shape=outs,
        in_specs=[hbm_spec] * 6,
        out_specs=(vmem_spec,) * 4,
        scratch_shapes=[
            vmem(big, F32), vmem(big, BF16), vmem(small, F32), vmem(small, BF16), vmem(big, F32), vmem(small, F32),
            vmem(big, BF16), vmem(small, BF16),
            vmem(big, BF16), vmem(small, BF16), vmem((16, 1, 128), F32), vmem((16, 1, 128), F32),
            vmem((64, 64, 128), BF16), vmem((128, 32, 128), BF16), vmem((128, 1, 128), F32), vmem((2, 1, 128), F32), vmem((4, 64, 128), BF16),
            vmem((2, 1024, 512), BF16), vmem((2, 1024, 512), BF16),
            vmem((2, 512, 512), BF16), vmem((512, 512), BF16), vmem((2, 512, 512), BF16),
            vmem((512, 512), BF16), vmem((512, 512), BF16), vmem((512, 512), F32),
            vmem((512, 1024), BF16), vmem((512, 512), BF16), vmem((512, 512), BF16),
            sem((6,)), sem((4,)), sem((4,)), sem((3,)), sem((5,)), sem((2,)), sem((2, 4)), sem((2, 4)), sem((2,)), sem((2,)), sem,
        ],
        compiler_params=pltpu.CompilerParams(collective_id=0, has_side_effects=True, vmem_limit_bytes=40 << 20),
        name='muon_exchange',
    )(*operands)
    return pl.pallas_call(
        store_kernel,
        out_shape=outs,
        in_specs=[vmem_spec] * 4,
        out_specs=(hbm_spec,) * 4,
        scratch_shapes=[sem((4,))],
        name='store_outputs',
    )(*(pltpu.with_memory_space_constraint(x, pltpu.VMEM) for x in updated))


def solution(mesh):
    block_spec = P('stage', 'data', 'model')

    def local_step(*args):
        return tuple(jnp.swapaxes(out, 1, 2) for out in local_update(*(jnp.swapaxes(arg, 1, 2) for arg in args)))

    return jax.shard_map(local_step, mesh=mesh, in_specs=(block_spec,) * 6, out_specs=(block_spec,) * 4, check_vma=False)
```
